32 devices in a mesh: span: 8 (over z, x), chord: 4 (over y, core).
Axes of the slice: x: 2, y: 2, z: 4, core: 2. Of those that a mesh axis runs over, the one named last changes fastest.
Arguments:
- fluid_state: float32 [4, 256, 128, 128], P(None, 'span', 'chord'), may hold values from -6 to 6
- shell_disp: float32 [3, 1024, 512], P(None, 'span', 'chord'), may hold values from -6 to 6
- shell_vel: float32 [3, 1024, 512], P(None, 'span', 'chord'), may hold values from -6 to 6
- owners: int32 [32768, 4], P(('span', 'chord')), may hold values from 0 to 31, all different within a row; in each aligned block of 1024 rows (0 to 1023, 1024 to 2047, ...) at most 256 rows name the same one
- node_local: int32 [32768, 4], P(('span', 'chord')), may hold values from 0 to 16383
- rbf_weight: float32 [32768, 4], P(('span', 'chord')), may hold values from 0.2 to 1
- normals: float32 [3, 32768], P(None, ('span', 'chord')), may hold values from -6 to 6
Outputs:
- fluid_next: float32 [4, 256, 128, 128], P(None, 'span', 'chord')
- interface_motion: float32 [6, 32768], P(None, ('span', 'chord'))
- disp_next: float32 [3, 1024, 512], P(None, 'span', 'chord')
- vel_next: float32 [3, 1024, 512], P(None, 'span', 'chord')
The draws below stay inside these ranges and needn't reach their ends.
Inputs may be any that keep to these rules, and one draw needn't show every extreme that they name: Each interface point names 4 different owners; the points of one device name no owner more than 256 times, a bound that some block reaches.
All inputs are finite; a program needn't handle non-finite values.
Results may differ from the reference program's by a relative error of at most 0.00007.
Values sent between devices are 32-bit elements; how exact they have to be, the bound alone decides.
No kernel may reach another device: no remote copies, remote signals or barrier semaphores. Data moves between devices by JAX's collectives and lax.ppermute only.
A program may use at most 64 MiB of HBM per device.

```python
import math
import jax
import jax.numpy as jnp
import numpy as np
from jax import lax

CX = 32
CY = 32
SX = 128
SY = 128
K = 4
NX = 256
NY = 128
NZ = 128
SNX = 1024
SNY = 512
POINTS = 32768
CAP = 256
N_SPAN = 8
N_CHORD = 4
DEVICES = 32


def plant(drawn, own_key, smallest, high):
    longest = drawn.shape.index(max(drawn.shape))
    spots = []
    for shift in (0, 1):
        where = [jax.random.randint(jax.random.fold_in(own_key, axis), (), 0, length) for axis, length in enumerate(drawn.shape)]
        where[longest] = (where[longest] + shift) % drawn.shape[longest]
        spots.append(tuple(where))
    return drawn.at[spots[0]].set(smallest).at[spots[1]].set(high)


def block_levels(rng, shape, pieces, smallest, high):
    def one(axis_at, shards_of):
        draws = jax.random.uniform(jax.random.fold_in(jax.random.fold_in(rng, 6), axis_at), (shards_of,), jnp.float32, smallest / len(pieces), high / len(pieces))
        return jnp.repeat(jnp.exp(draws), shape[axis_at] // shards_of).reshape((-1,) + (1,) * (len(shape) - axis_at - 1))

    level = one(*pieces[0])
    for cut in pieces[1:]:
        level = level * one(*cut)
    return level


def routed_block(stream_key, own, number, rows, count, top, reach, skew):
    sequence = jax.random.permutation(stream_key, count)
    packed, ordinary = load_shares(count, rows * top, reach, skew, True), load_shares(count, rows * top, reach, skew, False)
    places = jnp.arange(count)

    def named(sizes, turn):
        used = int((sizes > 0).sum())
        fixed = max(1, used // 4)
        passed = fixed + (places - fixed + turn * (used - fixed)) % max(1, count - fixed)
        return jnp.zeros((count,), jnp.int32).at[sequence[jnp.where(places < fixed, places, passed)]].set(jnp.asarray(sizes, jnp.int32))

    sizes = jnp.where(number % 4 == 0, named(packed, number // 4), named(ordinary, number - number // 4 - 1))
    mixed = jax.random.permutation(jax.random.fold_in(own, 3), count)
    giver, taker = mixed[0:count // 2 * 2:2], mixed[1:count // 2 * 2:2]
    slack = jnp.minimum(sizes[giver] - 1, reach - sizes[taker]) // 2
    slack = jnp.where((giver == sequence[0]) | (taker == sequence[0]) | (sizes[taker] == 0), 0, jnp.maximum(slack, 0))
    passed = jax.random.randint(jax.random.fold_in(own, 4), (count // 2,), 0, 1 << 20) % (slack + 1)
    sizes = sizes.at[giver].add(-passed).at[taker].add(passed)
    members = jnp.searchsorted(jnp.cumsum(sizes), jnp.arange(rows * top), side="right").astype(jnp.int32)
    grid = members.reshape(top, rows).T
    grid = grid[jax.random.permutation(jax.random.fold_in(own, 1), rows)]
    turn = jax.random.randint(jax.random.fold_in(own, 2), (rows, 1), 0, top)
    return jnp.take_along_axis(grid, (jnp.arange(top)[None, :] + turn) % top, axis=1)


def load_shares(amount, total, limit, skew, full):
    portions = [(1 << 20) // math.isqrt(rank ** skew) + 1 for rank in range(1, amount + 1)]
    largest = limit if full else min(limit, max(-(-total // amount), total * portions[0] // sum(portions)))
    least = 1 if total - largest >= amount - 1 else 0
    counts, spare = [largest] + [least] * (amount - 1), total - largest - least * (amount - 1)
    while spare > 0:
        movable = [i for i in range(1, amount) if counts[i] < largest] or [i for i in range(1, amount) if counts[i] < limit]
        whole, budget = sum([portions[i] for i in movable]), spare
        for i in movable:
            more = min(limit - counts[i], max(1, budget * portions[i] // whole), spare)
            counts[i] = counts[i] + more
            spare = spare - more
    return np.array(counts)


def normal_values(key, shape, width, bound, cuts=(), held_as=jnp.bfloat16):
    factor_of = block_levels(key, shape, cuts, -0.22, 0.18) if cuts else 1.0
    array = jax.random.normal(key, shape, jnp.float32) * width * factor_of
    return jnp.minimum(jnp.maximum(array, -bound), bound).astype(held_as)


def setup_inputs(seed: int = 0) -> dict:
    seeds = jax.random.split(jax.random.key(seed), 8)
    fluid_state = normal_values(seeds[0], (4, NX, NY, NZ), 1.0, 6.0, ((1, 8), (2, 4)), jnp.float32)
    shell_disp = normal_values(seeds[1], (3, SNX, SNY), 1.0, 6.0, ((1, 8), (2, 4)), jnp.float32)
    shell_vel = normal_values(seeds[2], (3, SNX, SNY), 1.0, 6.0, ((1, 8), (2, 4)), jnp.float32)
    owners_keys = jax.random.split(jax.random.fold_in(seeds[3], 1), POINTS // (CX * CY))
    owners_turns = jax.random.permutation(jax.random.fold_in(seeds[3], 3), POINTS // (CX * CY))
    owners = jax.vmap(lambda own, number: routed_block(jax.random.fold_in(seeds[3], 2), own, number, CX * CY, DEVICES, K, CAP, 2))(owners_keys, owners_turns).reshape((POINTS, K))
    node_local = plant(jax.random.randint(seeds[4], (POINTS, K), 0, SX * SY), jax.random.fold_in(seeds[4], 1), 0, (SX * SY) - 1).astype(jnp.int32)
    rbf_weight = jnp.clip(0.2 + 0.8 * jax.random.uniform(seeds[5], (POINTS, K), jnp.float32) ** block_levels(seeds[5], (POINTS, K), ((0, 32),), -0.2, 0.2), 0.2, 1.0)
    normals = normal_values(seeds[6], (3, POINTS), 1.0, 6.0, ((1, 32),), jnp.float32)
    return {"fluid_state": fluid_state, "shell_disp": shell_disp, "shell_vel": shell_vel, "owners": owners, "node_local": node_local, "rbf_weight": rbf_weight, "normals": normals}


flow_speed = 0.5
time_step = 0.4
stiffness = 0.5
damping = 0.2
shell_step = 0.3


def central(padded, direction):
    length = padded.shape[direction] - 6

    def window(offset):
        return lax.slice_in_dim(padded, 3 + offset, 3 + offset + length, axis=direction)

    return (45.0 * (window(1) - window(-1)) - 9.0 * (window(2) - window(-2)) + (window(3) - window(-3))) / 60.0


def wall_padded(fluid, wall_motion):
    mirror = fluid[:, :, :, 2::-1]
    moving = 2.0 * wall_motion[:, :, :, None] - mirror[1:]
    lower_ghost = jnp.concatenate([mirror[:1], moving], axis=0)
    upper_ghost = jnp.zeros(fluid.shape[:3] + (3,), fluid.dtype)
    return jnp.concatenate([lower_ghost, fluid, upper_ghost], axis=3)


def fluid_rates(span_padded, chord_padded, normal_padded):
    along_span = central(span_padded, 1)
    along_chord = central(chord_padded, 2)
    along_normal = central(normal_padded[0::3], 3)
    rate_p = -flow_speed * along_span[0] - (along_span[1] + along_chord[1] + along_normal[1])
    rate_u = -flow_speed * along_span[1] - along_span[0]
    rate_v = -flow_speed * along_span[2] - along_chord[0]
    rate_w = -flow_speed * along_span[3] - along_normal[0]
    return jnp.stack([rate_p, rate_u, rate_v, rate_w])


def laplacian(padded):
    center = padded[:, 1:-1, 1:-1]
    return padded[:, 2:, 1:-1] + padded[:, :-2, 1:-1] + padded[:, 1:-1, 2:] + padded[:, 1:-1, :-2] - 4.0 * center


def reference(fluid_state, shell_disp, shell_vel, owners, node_local, rbf_weight, normals):
    points = jnp.arange(CX * CY * N_SPAN * N_CHORD, dtype=jnp.int32)
    owner_block = points // (CX * CY)
    inside = points % (CX * CY)
    point_x = (owner_block // N_CHORD) * CX + inside // CY
    point_y = (owner_block % N_CHORD) * CY + inside % CY
    node_x = (owners // N_CHORD) * SX + node_local // SY
    node_y = (owners % N_CHORD) * SY + node_local % SY
    stacked = jnp.concatenate([shell_disp, shell_vel], axis=0)
    motion = stacked[:, node_x, node_y]
    interface_motion = jnp.sum(motion * rbf_weight[None], axis=2)
    wall_motion = jnp.zeros((3, CX * N_SPAN, CY * N_CHORD), jnp.float32).at[:, point_x, point_y].set(interface_motion[3:])
    span_padded = jnp.pad(fluid_state, ((0, 0), (3, 3), (0, 0), (0, 0)))
    chord_padded = jnp.pad(fluid_state[0::2], ((0, 0), (0, 0), (3, 3), (0, 0)))
    normal_padded = wall_padded(fluid_state, wall_motion)
    fluid_next = fluid_state + time_step * fluid_rates(span_padded, chord_padded, normal_padded)
    pressure = fluid_next[0, point_x, point_y, 0]
    surface_load = normals * pressure[None]
    contrib = surface_load[:, :, None] * rbf_weight[None]
    shell_force = jnp.zeros((3, SX * N_SPAN, SY * N_CHORD), jnp.float32).at[:, node_x, node_y].add(contrib)
    bending = laplacian(jnp.pad(shell_disp, ((0, 0), (1, 1), (1, 1))))
    acceleration = stiffness * bending + shell_force - damping * shell_vel
    vel_next = shell_vel + shell_step * acceleration
    disp_next = shell_disp + shell_step * vel_next
    return fluid_next, interface_motion, disp_next, vel_next
```

```python
import functools

import jax
import jax.numpy as jnp
from jax import lax
from jax.experimental import pallas as pl
from jax.experimental.pallas import tpu as pltpu
from jax.sharding import PartitionSpec as P

flow_speed = 0.5
time_step = 0.4
stiffness = 0.5
damping = 0.2
shell_step = 0.3

AXES = ("span", "chord")
LANES = 128
f32 = jnp.float32
bf16 = jnp.bfloat16
i32 = jnp.int32
NT = (((1,), (1,)), ((), ()))
TN = (((0,), (0,)), ((), ()))
NN = (((1,), (0,)), ((), ()))
HIGHEST = lax.Precision.HIGHEST


def dot(a, b, dims, precision=None):
    return lax.dot_general(a, b, dims, precision=precision, preferred_element_type=f32)


def iota(shape, dim):
    return lax.broadcasted_iota(i32, shape, dim)


def split(value):
    high = value.astype(bf16)
    low = (value - high.astype(f32)).astype(bf16)
    return high, low


def call(kernel, outs, *args, name, flops=1_000_000, **kw):
    single = not isinstance(outs, (list, tuple))
    space = pl.BlockSpec(memory_space=pltpu.VMEM)
    kw.setdefault("in_specs", [space] * len(args))
    kw.setdefault("out_specs", space if single else [space] * len(outs))
    nbytes = sum(a.size * a.dtype.itemsize for a in args)
    return pl.pallas_call(
        kernel,
        out_shape=outs,
        name=name,
        cost_estimate=pl.CostEstimate(flops=flops, transcendentals=0, bytes_accessed=nbytes),
        **kw,
    )(*args)


def route_kernel(devices, capacity, own_ref, node_ref, req_ref, dest_ref):
    stencil, points = own_ref.shape
    blocks = points // LANES
    rows = req_ref.shape[0]
    member = []
    for b in range(blocks):
        ids = iota((devices, LANES), 0)
        hit = jnp.zeros((devices, LANES), f32)
        for k in range(stencil):
            hit = jnp.where(own_ref[k : k + 1, b * LANES : (b + 1) * LANES] == ids, 1.0, hit)
        member.append(hit)
    stacked = jnp.concatenate(member, axis=0).astype(bf16)
    source = iota((LANES, 2 * LANES), 0)
    target = iota((LANES, 2 * LANES), 1)
    table = jnp.where((source < target) | (target >= LANES), 1.0, 0.0).astype(bf16)
    counted = dot(stacked, table, NN)
    offset = jnp.zeros((devices, LANES), f32)
    for b in range(blocks):
        part = counted[b * devices : (b + 1) * devices]
        rank = part[:, :LANES] + offset
        offset = offset + part[:, LANES:]
        ids = iota((devices, LANES), 0)
        for k in range(stencil):
            own = own_ref[k : k + 1, b * LANES : (b + 1) * LANES]
            mine = jnp.sum(jnp.where(own == ids, rank, 0.0), axis=0, keepdims=True)
            dest_ref[k : k + 1, b * LANES : (b + 1) * LANES] = own * capacity + mine.astype(i32)
    total = jnp.zeros((2 * rows, LANES), f32)
    for k in range(stencil):
        dest = dest_ref[k : k + 1, :]
        node = node_ref[k : k + 1, :]
        place = iota((rows, points), 0) == dest // LANES
        upper = (node // LANES + 1).astype(f32)
        lower = (node % LANES).astype(f32)
        left = jnp.concatenate(
            [jnp.where(place, upper, 0.0), jnp.where(place, lower, 0.0)], axis=0
        ).astype(bf16)
        right = jnp.where(iota((LANES, points), 0) == dest % LANES, 1.0, 0.0).astype(bf16)
        total = total + dot(left, right, NT)
    req_ref[...] = (total[:rows] * LANES + total[rows:]).astype(i32)


def slots_kernel(dest_ref, weight_ref, disp_ref, vel_ref, slots_ref, table_ref):
    stencil, points = dest_ref.shape
    rows = slots_ref.shape[1]
    total = jnp.zeros((4 * rows, LANES), f32)
    point = iota((1, points), 1)
    point_a = (point // LANES).astype(f32)
    point_b = (point % LANES).astype(f32)
    for k in range(stencil):
        dest = dest_ref[k : k + 1, :]
        high, low = split(weight_ref[k : k + 1, :])
        place = iota((rows, points), 0) == dest // LANES
        parts = [point_a, point_b, high.astype(f32), low.astype(f32)]
        left = jnp.concatenate([jnp.where(place, part, 0.0) for part in parts], axis=0)
        right = jnp.where(iota((LANES, points), 0) == dest % LANES, 1.0, 0.0).astype(bf16)
        total = total + dot(left.astype(bf16), right, NT)
    slots_ref[0] = total[:rows]
    slots_ref[1] = total[rows : 2 * rows]
    slots_ref[2] = total[2 * rows : 3 * rows] + total[3 * rows :]
    for c in range(6):
        field = disp_ref[c] if c < 3 else vel_ref[c - 3]
        high, low = split(field.T)
        width = field.shape[1]
        table_ref[c * width : (c + 1) * width, : field.shape[0]] = high
        table_ref[c * width : (c + 1) * width, field.shape[0] :] = low


def pair(ref, first, start=None):
    if start is None:
        return jnp.concatenate([ref[pl.ds(first, 1), :], ref[pl.ds(first + 1, 1), :]], axis=1)
    return jnp.concatenate(
        [ref[start, pl.ds(first, 1), :], ref[start, pl.ds(first + 1, 1), :]], axis=1
    )


def position(chunk_rows, channels, rows, channel, row):
    if chunk_rows:
        return (row // chunk_rows) * (channels * chunk_rows) + channel * chunk_rows + row % chunk_rows
    return channel * rows + row


def fetch_kernel(chunk_rows, asked_ref, table_ref, out_ref):
    rows = asked_ref.shape[0]
    nodes = table_ref.shape[1] // 2
    width = table_ref.shape[0] // 6

    def step(t, carry):
        asked = pair(asked_ref, 2 * t)
        upper = asked // LANES - 1
        lower = asked % LANES
        hot = jnp.where(iota((nodes, 2 * LANES), 0) == upper, 1.0, 0.0).astype(bf16)
        picked = dot(table_ref[...], jnp.concatenate([hot, hot], axis=0), NN)
        keep = iota((width, 2 * LANES), 0) == lower
        for c in range(6):
            found = jnp.sum(
                jnp.where(keep, picked[c * width : (c + 1) * width], 0.0), axis=0, keepdims=True
            )
            for half in range(2):
                at = position(chunk_rows, 6, rows, c, 2 * t + half)
                out_ref[pl.ds(at, 1), :] = found[:, half * LANES : (half + 1) * LANES]
        return carry

    lax.fori_loop(0, rows // 2, step, 0)


def meet_kernel(
    chunk_rows, factor, got_ref, slots_ref, base_ref, normals_ref, motion_ref, wall_ref, out_ref,
    hot_ref,
):
    rows = slots_ref.shape[1]
    blocks = base_ref.shape[0]

    def gather(t, total):
        weight = pair(slots_ref, 2 * t, 2)
        mine = iota((blocks, 2 * LANES), 0).astype(f32) == pair(slots_ref, 2 * t, 0)
        hot = jnp.where(
            iota((LANES, 2 * LANES), 0).astype(f32) == pair(slots_ref, 2 * t, 1), 1.0, 0.0
        ).astype(bf16)
        hot_ref[t] = hot
        left = []
        for c in range(6):
            first = position(chunk_rows, 6, rows, c, 2 * t)
            second = position(chunk_rows, 6, rows, c, 2 * t + 1)
            value = jnp.concatenate(
                [got_ref[pl.ds(first, 1), :], got_ref[pl.ds(second, 1), :]], axis=1
            )
            for part in split(value * weight):
                left.append(jnp.where(mine, part.astype(f32), 0.0))
        left = jnp.concatenate(left, axis=0).astype(bf16)
        return total + dot(left, hot, NT)

    total = lax.fori_loop(0, rows // 2, gather, jnp.zeros((12 * blocks, LANES), f32))
    for c in range(6):
        value = total[2 * c * blocks : (2 * c + 1) * blocks] + total[(2 * c + 1) * blocks : (2 * c + 2) * blocks]
        for a in range(blocks):
            motion_ref[c : c + 1, a * LANES : (a + 1) * LANES] = value[a : a + 1]
    wall = value
    wall_ref[...] = wall
    pressure = base_ref[...] + factor * wall
    left = []
    for c in range(3):
        normal = jnp.concatenate(
            [normals_ref[c : c + 1, a * LANES : (a + 1) * LANES] for a in range(blocks)], axis=0
        )
        left.extend(part.astype(f32) for part in split(normal * pressure))
    left = jnp.concatenate(left, axis=0).astype(bf16)

    def spread(t, carry):
        weight = pair(slots_ref, 2 * t, 2)
        mine = iota((blocks, 2 * LANES), 0).astype(f32) == pair(slots_ref, 2 * t, 0)
        seen = dot(left, hot_ref[t], NN)
        for c in range(3):
            both = seen[2 * c * blocks : (2 * c + 1) * blocks] + seen[(2 * c + 1) * blocks : (2 * c + 2) * blocks]
            load = weight * jnp.sum(jnp.where(mine, both, 0.0), axis=0, keepdims=True)
            for half in range(2):
                at = position(chunk_rows, 3, rows, c, 2 * t + half)
                out_ref[pl.ds(at, 1), :] = load[:, half * LANES : (half + 1) * LANES]
        return carry

    lax.fori_loop(0, rows // 2, spread, 0)


def force_kernel(chunk_rows, got_ref, asked_ref, base_ref, disp_ref, disp_out, vel_out, total_ref):
    rows = asked_ref.shape[0]
    nodes, width = disp_ref.shape[1], disp_ref.shape[2]
    half_nodes = nodes // 2
    total_ref[...] = jnp.zeros_like(total_ref)

    def step(t, carry):
        asked = pair(asked_ref, 2 * t)
        upper = asked // LANES - 1
        lower = asked % LANES
        second = upper >= half_nodes
        place = iota((half_nodes, 2 * LANES), 0) == jnp.where(second, upper - half_nodes, upper)
        hot = jnp.where(
            iota((2 * width, 2 * LANES), 0) == jnp.where(second, lower + width, lower), 1.0, 0.0
        ).astype(bf16)
        left = []
        for c in range(3):
            one = position(chunk_rows, 3, rows, c, 2 * t)
            two = position(chunk_rows, 3, rows, c, 2 * t + 1)
            value = jnp.concatenate(
                [got_ref[pl.ds(one, 1), :], got_ref[pl.ds(two, 1), :]], axis=1
            )
            for part in split(value):
                left.append(jnp.where(place, part.astype(f32), 0.0))
        left = jnp.concatenate(left, axis=0).astype(bf16)
        total_ref[...] += dot(left, hot, NT)
        return carry

    lax.fori_loop(0, rows // 2, step, 0)
    for c in range(3):
        for h in range(2):
            first = total_ref[2 * c * half_nodes : (2 * c + 1) * half_nodes, h * width : (h + 1) * width]
            second = total_ref[(2 * c + 1) * half_nodes : (2 * c + 2) * half_nodes, h * width : (h + 1) * width]
            at = slice(h * half_nodes, (h + 1) * half_nodes)
            vel_next = base_ref[c, at, :] + shell_step * (first + second)
            vel_out[c, at, :] = vel_next
            disp_out[c, at, :] = disp_ref[c, at, :] + shell_step * vel_next


def pack_kernel(
    disp_ref, fluid_ref, span_last, span_first, chord_last, chord_first, edges, sems
):
    fields, cells_x, cells_y, _ = fluid_ref.shape
    nodes, width = disp_ref.shape[1], disp_ref.shape[2]
    copies = []

    def copy(source, target):
        one = pltpu.make_async_copy(source, target, sems.at[len(copies)])
        one.start()
        copies.append(one)

    for c in range(fields):
        copy(fluid_ref.at[c, pl.ds(cells_x - 3, 3)], span_last.at[pl.ds(3 * c, 3)])
        copy(fluid_ref.at[c, pl.ds(0, 3)], span_first.at[pl.ds(3 * c, 3)])
    for n, c in enumerate((0, 2)):
        copy(fluid_ref.at[c, :, pl.ds(cells_y - 8, 8)], chord_last.at[pl.ds(n * cells_x, cells_x)])
        copy(fluid_ref.at[c, :, pl.ds(0, 8)], chord_first.at[pl.ds(n * cells_x, cells_x)])
    edges[...] = jnp.zeros_like(edges)
    for c in range(3):
        field = disp_ref[c]
        edges[0, c : c + 1, :] = field[nodes - 1 :, :]
        edges[1, c : c + 1, :] = field[:1, :]
        turned = field.T
        edges[2, c : c + 1, :] = turned[width - 1 :, :]
        edges[3, c : c + 1, :] = turned[:1, :]
    copy(edges.at[0], span_last.at[3 * fields, pl.ds(0, 8)])
    copy(edges.at[1], span_first.at[3 * fields, pl.ds(0, 8)])
    copy(edges.at[2], chord_last.at[2 * cells_x])
    copy(edges.at[3], chord_first.at[2 * cells_x])
    for one in copies:
        one.wait()


def coef(distance):
    size = jnp.abs(distance)
    value = jnp.where(size == 1, 45.0, jnp.where(size == 2, -9.0, jnp.where(size == 3, 1.0, 0.0)))
    return jnp.where(distance < 0, -value, value)


def flow_kernel(
    disp_ref, vel_ref, fluid_ref, before_x, after_x, before_y, after_y,
    next_ref, surface_ref, shell_ref, wide, tall, edges, sems,
):
    fields, cells_x, cells_y, length = fluid_ref.shape
    step = pl.program_id(0)
    chunk = next_ref.shape[1]
    nodes, width = disp_ref.shape[1], disp_ref.shape[2]

    @pl.when(step == 0)
    def _():
        copies = []

        def copy(source, target):
            one = pltpu.make_async_copy(source, target, sems.at[len(copies)])
            one.start()
            copies.append(one)

        for c in range(fields):
            copy(fluid_ref.at[c], wide.at[c, pl.ds(3, cells_x)])
            copy(before_x.at[pl.ds(3 * c, 3)], wide.at[c, pl.ds(0, 3)])
            copy(after_x.at[pl.ds(3 * c, 3)], wide.at[c, pl.ds(3 + cells_x, 3)])
        for n, c in enumerate((0, 2)):
            copy(fluid_ref.at[c], tall.at[n, :, pl.ds(8, cells_y)])
            copy(before_y.at[pl.ds(n * cells_x, cells_x)], tall.at[n, :, pl.ds(0, 8)])
            copy(after_y.at[pl.ds(n * cells_x, cells_x)], tall.at[n, :, pl.ds(8 + cells_y, 8)])
        copy(before_x.at[3 * fields, pl.ds(0, 8)], edges.at[0])
        copy(after_x.at[3 * fields, pl.ds(0, 8)], edges.at[1])
        copy(before_y.at[2 * cells_x], edges.at[2])
        copy(after_y.at[2 * cells_x], edges.at[3])
        for one in copies:
            one.wait()
        row = iota((nodes, width), 0)
        lane = iota((nodes, width), 1)
        channel = iota((8, width), 0)
        for c in range(3):
            field = disp_ref[c]
            only = channel == c
            left = dot(
                jnp.where(only, edges[2], 0.0), jnp.where(iota((8, width), 1) == 0, 1.0, 0.0), TN, HIGHEST
            )
            right = dot(
                jnp.where(only, edges[3], 0.0), jnp.where(iota((8, width), 1) == width - 1, 1.0, 0.0), TN, HIGHEST
            )
            above = jnp.where(row == 0, edges[0, c : c + 1, :], pltpu.roll(field, 1, 0))
            below = jnp.where(row == nodes - 1, edges[1, c : c + 1, :], pltpu.roll(field, nodes - 1, 0))
            west = jnp.where(lane == 0, left, pltpu.roll(field, 1, 1))
            east = jnp.where(lane == width - 1, right, pltpu.roll(field, width - 1, 1))
            bending = above + below + west + east - 4.0 * field
            vel = vel_ref[c]
            shell_ref[c] = vel + shell_step * (stiffness * bending - damping * vel)

    source = iota((length, length), 0)
    target = iota((length, length), 1)
    inner = coef(source - target)
    ghost = jnp.where(source < 3, coef(-(source + 1 + target)), 0.0)
    pressure_table = (inner + ghost).astype(bf16)
    normal_table = (inner - ghost).astype(bf16)
    first = step * chunk
    flat = chunk * cells_y

    def normal(field, table):
        value = wide[field, pl.ds(first + 3, chunk)].reshape(flat, length)
        high, low = split(value)
        return ((dot(high, table, NN) + dot(low, table, NN)) * (1.0 / 60.0)).reshape(
            chunk, cells_y, length
        )

    def along_x(field):
        def window(offset):
            return wide[field, pl.ds(first + 3 + offset, chunk)]

        return (
            45.0 * (window(1) - window(-1)) - 9.0 * (window(2) - window(-2)) + (window(3) - window(-3))
        ) * (1.0 / 60.0)

    def along_y(slot):
        def window(offset):
            return tall[slot, pl.ds(first, chunk), 8 + offset : 8 + offset + cells_y, :]

        return (
            45.0 * (window(1) - window(-1)) - 9.0 * (window(2) - window(-2)) + (window(3) - window(-3))
        ) * (1.0 / 60.0)

    def old(field):
        return wide[field, pl.ds(first + 3, chunk)]

    x_p = along_x(0)
    x_u = along_x(1)
    p_next = old(0) + time_step * (-flow_speed * x_p - (x_u + along_y(1) + normal(3, normal_table)))
    next_ref[0] = p_next
    next_ref[1] = old(1) + time_step * (-flow_speed * x_u - x_p)
    next_ref[2] = old(2) + time_step * (-flow_speed * along_x(2) - along_y(0))
    next_ref[3] = old(3) + time_step * (-flow_speed * along_x(3) - normal(0, pressure_table))
    lead = jnp.where((iota((8, length), 0) == 0) & (iota((8, length), 1) == 0), 1.0, 0.0)
    found = dot(lead, p_next.reshape(flat, length), NT, HIGHEST)
    for b in range(flat // LANES):
        surface_ref[pl.ds(step * (flat // LANES) + b, 1), :] = found[:1, b * LANES : (b + 1) * LANES]


def wall_kernel(wall_ref, next_in, next_out):
    length = next_in.shape[3]
    chunk, cells_y = next_in.shape[1], next_in.shape[2]
    step = pl.program_id(0)
    per = chunk * cells_y // LANES
    target = iota((8, length), 1)
    row = jnp.zeros((8, length), f32)
    for j in range(3):
        row = row + coef(-(j + 1 + target))
    row = jnp.where(iota((8, length), 0) == 0, row * (-2.0 * time_step / 60.0), 0.0)
    for b in range(per):
        wall = jnp.where(
            iota((8, LANES), 0) == 0, wall_ref[pl.ds(step * per + b, 1), :], 0.0
        )
        added = dot(wall, row, TN, HIGHEST)
        xs = LANES // cells_y
        at = slice(b * xs, (b + 1) * xs)
        next_out[0, at] = next_in[0, at] + added.reshape(xs, cells_y, length)


def exchange(value, devices, channels, chunk_rows, rows, capacity):
    if chunk_rows:
        shape = (devices, 1, channels * chunk_rows * LANES)
        got = lax.all_to_all(value.reshape(shape), AXES, split_axis=0, concat_axis=0, tiled=True)
        return got.reshape(channels * rows, LANES)
    value = value.reshape(channels, devices, capacity).transpose(1, 0, 2)
    got = lax.all_to_all(value, AXES, split_axis=0, concat_axis=0, tiled=True)
    return got.transpose(1, 0, 2).reshape(channels * rows, LANES)


def body(fluid_state, shell_disp, shell_vel, owners, node_local, rbf_weight, normals):
    span_count = lax.axis_size("span")
    chord_count = lax.axis_size("chord")
    devices = span_count * chord_count
    points, stencil = owners.shape
    capacity = max(2, (2 * points * stencil + devices - 1) // devices)
    rows = devices * capacity // LANES
    chunk_rows = capacity // LANES if capacity % LANES == 0 else 0
    blocks = points // LANES
    fields, cells_x, cells_y, length = fluid_state.shape
    _, nodes, width = shell_disp.shape
    sds = jax.ShapeDtypeStruct
    vmem = pl.BlockSpec(memory_space=pltpu.VMEM)
    hbm = pl.BlockSpec(memory_space=pl.ANY)

    requests, dest = call(
        functools.partial(route_kernel, devices, capacity),
        [sds((rows, LANES), i32), sds((stencil, points), i32)],
        owners.T,
        node_local.T,
        name="route",
    )
    asked = exchange(requests, devices, 1, chunk_rows, rows, capacity)

    slots, table = call(
        slots_kernel,
        [sds((3, rows, LANES), f32), sds((6 * width, 2 * nodes), bf16)],
        dest,
        rbf_weight.T,
        shell_disp,
        shell_vel,
        name="slots",
        flops=200_000_000,
    )

    span_shape = sds((3 * fields + 1, cells_y, length), f32)
    chord_shape = sds((2 * cells_x + 1, 8, length), f32)
    span_last, span_first, chord_last, chord_first = call(
        pack_kernel,
        [span_shape, span_shape, chord_shape, chord_shape],
        shell_disp,
        fluid_state,
        name="pack",
        in_specs=[vmem, hbm],
        out_specs=[hbm] * 4,
        scratch_shapes=[
            pltpu.VMEM((4, 8, width), f32),
            pltpu.SemaphoreType.DMA((2 * fields + 8,)),
        ],
    )

    def shifted(last, leading, axis, size):
        up = [(i, i + 1) for i in range(size - 1)]
        down = [(i + 1, i) for i in range(size - 1)]
        return lax.ppermute(last, axis, up), lax.ppermute(leading, axis, down)

    before_x, after_x = shifted(span_last, span_first, "span", span_count)
    before_y, after_y = shifted(chord_last, chord_first, "chord", chord_count)

    chunk = LANES // cells_y
    flow_next, surface, shell_base = call(
        flow_kernel,
        [
            sds(fluid_state.shape, f32),
            sds((blocks, LANES), f32),
            sds(shell_disp.shape, f32),
        ],
        shell_disp,
        shell_vel,
        fluid_state,
        before_x,
        after_x,
        before_y,
        after_y,
        name="flow",
        flops=300_000_000,
        grid=(cells_x // chunk,),
        in_specs=[vmem, vmem, hbm, hbm, hbm, hbm, hbm],
        out_specs=[
            pl.BlockSpec((fields, chunk, cells_y, length), lambda i: (0, i, 0, 0)),
            pl.BlockSpec((blocks, LANES), lambda i: (0, 0)),
            pl.BlockSpec(shell_disp.shape, lambda i: (0, 0, 0)),
        ],
        scratch_shapes=[
            pltpu.VMEM((fields, cells_x + 6, cells_y, length), f32),
            pltpu.VMEM((2, cells_x, cells_y + 16, length), f32),
            pltpu.VMEM((4, 8, width), f32),
            pltpu.SemaphoreType.DMA((3 * fields + 10,)),
        ],
    )

    picked = call(
        functools.partial(fetch_kernel, chunk_rows),
        sds((6 * rows, LANES), f32),
        asked,
        table,
        name="fetch",
        flops=3_000_000_000,
    )
    replies = exchange(picked, devices, 6, chunk_rows, rows, capacity)

    wall_first = 2.0 * (-45.0 + 9.0 - 1.0) / 60.0
    interface_motion, wall, loads = call(
        functools.partial(meet_kernel, chunk_rows, -time_step * wall_first),
        [
            sds((6, points), f32),
            sds((blocks, LANES), f32),
            sds((3 * rows, LANES), f32),
        ],
        replies,
        slots,
        surface,
        normals,
        name="meet",
        flops=300_000_000,
        scratch_shapes=[pltpu.VMEM((rows // 2, LANES, 2 * LANES), bf16)],
    )
    arrived = exchange(loads, devices, 3, chunk_rows, rows, capacity)

    big = cells_x // 4
    block = pl.BlockSpec((1, big, cells_y, length), lambda i: (0, i, 0, 0))
    fluid_next = call(
        wall_kernel,
        sds(fluid_state.shape, f32),
        wall,
        flow_next,
        name="wall",
        flops=100_000_000,
        grid=(4,),
        in_specs=[vmem, block],
        out_specs=block,
        input_output_aliases={1: 0},
    )

    disp_next, vel_next = call(
        functools.partial(force_kernel, chunk_rows),
        [sds(shell_disp.shape, f32), sds(shell_vel.shape, f32)],
        arrived,
        asked,
        shell_base,
        shell_disp,
        name="force",
        flops=3_000_000_000,
        scratch_shapes=[pltpu.VMEM((3 * nodes, 2 * width), f32)],
    )
    return (fluid_next, interface_motion, disp_next, vel_next)


def solution(mesh):
    placed = (
        P(None, "span", "chord", None),
        P(None, "span", "chord"),
        P(None, "span", "chord"),
        P(AXES, None),
        P(AXES, None),
        P(AXES, None),
        P(None, AXES),
    )
    return jax.shard_map(
        body,
        mesh=mesh,
        in_specs=placed,
        out_specs=(
            P(None, "span", "chord", None),
            P(None, AXES),
            P(None, "span", "chord"),
            P(None, "span", "chord"),
        ),
        check_vma=False,
    )
```

```python
import functools

import jax
import jax.numpy as jnp
from jax import lax
from jax.experimental import pallas as pl
from jax.experimental.pallas import tpu as pltpu
from jax.sharding import PartitionSpec as P


flow_speed = 0.5
time_step = 0.4
stiffness = 0.5
damping = 0.2
shell_step = 0.3

AXES = ("span", "chord")
LANES = 128
f32 = jnp.float32
bf16 = jnp.bfloat16
i32 = jnp.int32
NT = (((1,), (1,)), ((), ()))
TN = (((0,), (0,)), ((), ()))
NN = (((1,), (0,)), ((), ()))


def dot(a, b, dims, precision=None):
    return lax.dot_general(a, b, dims, precision=precision, preferred_element_type=f32)


def iota(shape, dim):
    return lax.broadcasted_iota(i32, shape, dim)


def split(value):
    high = value.astype(bf16)
    low = (value - high.astype(f32)).astype(bf16)
    return high, low


def near(value):
    return pltpu.with_memory_space_constraint(value, pltpu.VMEM)


def call(kernel, outs, *args, flops=1_000_000, held=(), **kw):
    single = not isinstance(outs, (list, tuple))
    space = pl.BlockSpec(memory_space=pltpu.VMEM)
    kw.setdefault("in_specs", [space] * len(args))
    args = [near(a) if n in held else a for n, a in enumerate(args)]
    kw.setdefault("out_specs", space if single else [space] * len(outs))
    nbytes = sum(a.size * a.dtype.itemsize for a in args)
    return pl.pallas_call(
        kernel,
        out_shape=outs,
        cost_estimate=pl.CostEstimate(flops=flops, transcendentals=0, bytes_accessed=nbytes),
        **kw,
    )(*args)


def route_kernel(devices, capacity, own_ref, node_ref, req_ref, dest_ref):
    stencil, points = own_ref.shape
    blocks = points // LANES
    rows = req_ref.shape[0]
    member = []
    for b in range(blocks):
        ids = iota((devices, LANES), 0)
        hit = jnp.zeros((devices, LANES), f32)
        for k in range(stencil):
            hit = jnp.where(own_ref[k : k + 1, b * LANES : (b + 1) * LANES] == ids, 1.0, hit)
        member.append(hit)
    stacked = jnp.concatenate(member, axis=0).astype(bf16)
    source = iota((LANES, 2 * LANES), 0)
    target = iota((LANES, 2 * LANES), 1)
    table = jnp.where((source < target) | (target >= LANES), 1.0, 0.0).astype(bf16)
    counted = dot(stacked, table, NN)
    offset = jnp.zeros((devices, LANES), f32)
    for b in range(blocks):
        part = counted[b * devices : (b + 1) * devices]
        rank = part[:, :LANES] + offset
        offset = offset + part[:, LANES:]
        ids = iota((devices, LANES), 0)
        for k in range(stencil):
            own = own_ref[k : k + 1, b * LANES : (b + 1) * LANES]
            mine = jnp.sum(jnp.where(own == ids, rank, 0.0), axis=0, keepdims=True)
            dest_ref[k : k + 1, b * LANES : (b + 1) * LANES] = own * capacity + mine.astype(i32)
    total = jnp.zeros((2 * rows, LANES), f32)
    for k in range(stencil):
        dest = dest_ref[k : k + 1, :]
        node = node_ref[k : k + 1, :]
        place = iota((rows, points), 0) == dest // LANES
        upper = (node // LANES + 1).astype(f32)
        lower = (node % LANES).astype(f32)
        left = jnp.concatenate(
            [jnp.where(place, upper, 0.0), jnp.where(place, lower, 0.0)], axis=0
        ).astype(bf16)
        right = jnp.where(iota((LANES, points), 0) == dest % LANES, 1.0, 0.0).astype(bf16)
        total = total + dot(left, right, NT)
    req_ref[...] = (total[:rows] * LANES + total[rows:]).astype(i32)


def slots_kernel(dest_ref, weight_ref, slots_ref):
    stencil, points = dest_ref.shape
    rows = slots_ref.shape[1]
    total = jnp.zeros((4 * rows, LANES), f32)
    point = iota((1, points), 1)
    point_a = (point // LANES).astype(f32)
    point_b = (point % LANES).astype(f32)
    for k in range(stencil):
        dest = dest_ref[k : k + 1, :]
        high, low = split(weight_ref[k : k + 1, :])
        place = iota((rows, points), 0) == dest // LANES
        parts = [point_a, point_b, high.astype(f32), low.astype(f32)]
        left = jnp.concatenate([jnp.where(place, part, 0.0) for part in parts], axis=0)
        right = jnp.where(iota((LANES, points), 0) == dest % LANES, 1.0, 0.0).astype(bf16)
        total = total + dot(left.astype(bf16), right, NT)
    slots_ref[0] = total[:rows]
    slots_ref[1] = total[rows : 2 * rows]
    slots_ref[2] = total[2 * rows : 3 * rows] + total[3 * rows :]


def table_kernel(disp_ref, vel_ref, table_ref):
    nodes, width = disp_ref.shape[1], disp_ref.shape[2]
    half = width // 2
    for c in range(6):
        field = disp_ref[c] if c < 3 else vel_ref[c - 3]
        for n, part in enumerate(split(field.T)):
            for h in range(2):
                first = (6 * n + c) * half
                table_ref[first : first + half, h * nodes : (h + 1) * nodes] = part[
                    h * half : (h + 1) * half
                ]


def pair(ref, first, start=None):
    if start is None:
        return jnp.concatenate([ref[pl.ds(first, 1), :], ref[pl.ds(first + 1, 1), :]], axis=1)
    return jnp.concatenate(
        [ref[start, pl.ds(first, 1), :], ref[start, pl.ds(first + 1, 1), :]], axis=1
    )


def position(chunk_rows, channels, rows, channel, row):
    if chunk_rows:
        return (row // chunk_rows) * (channels * chunk_rows) + channel * chunk_rows + row % chunk_rows
    return channel * rows + row


def fetch_kernel(chunk_rows, group, asked_ref, table_ref, out_ref):
    rows = asked_ref.shape[0]
    half = table_ref.shape[0] // 12
    double = table_ref.shape[1]
    nodes = double // 2

    def step(g, carry):
        for s in range(group):
            t = g * group + s
            asked = pair(asked_ref, 2 * t)
            lower = asked % LANES
            upper = asked // LANES - 1
            second = lower >= half
            at = jnp.where(upper < 0, -1, jnp.where(second, upper + nodes, upper))
            hot = jnp.where(iota((double, 2 * LANES), 0) == at, 1.0, 0.0).astype(bf16)
            picked = dot(table_ref[...], hot, NN)
            picked = picked[: 6 * half] + picked[6 * half :]
            keep = iota((half, 2 * LANES), 0) == jnp.where(second, lower - half, lower)
            for c in range(6):
                found = jnp.sum(
                    jnp.where(keep, picked[c * half : (c + 1) * half], 0.0), axis=0, keepdims=True
                )
                for h in range(2):
                    to = position(chunk_rows, 6, rows, c, 2 * t + h)
                    out_ref[pl.ds(to, 1), :] = found[:, h * LANES : (h + 1) * LANES]
        return carry

    lax.fori_loop(0, rows // (2 * group), step, 0)


def meet_kernel(
    chunk_rows, group, factor, got_ref, slots_ref, base_ref, normals_ref, motion_ref, wall_ref, out_ref,
    hot_ref,
):
    rows = slots_ref.shape[1]
    blocks = base_ref.shape[0]

    def gather(g, total):
        lefts, hots = [], []
        for s in range(group):
            row = g * group + s
            weight = slots_ref[2, pl.ds(row, 1), :]
            mine = iota((blocks, LANES), 0).astype(f32) == slots_ref[0, pl.ds(row, 1), :]
            hot = jnp.where(
                iota((LANES, LANES), 0).astype(f32) == slots_ref[1, pl.ds(row, 1), :], 1.0, 0.0
            ).astype(bf16)
            left = []
            for c in range(6):
                value = got_ref[pl.ds(position(chunk_rows, 6, rows, c, row), 1), :]
                for part in split(value * weight):
                    left.append(jnp.where(mine, part.astype(f32), 0.0))
            lefts.append(jnp.concatenate(left, axis=0).astype(bf16))
            hots.append(hot)
        hot = jnp.concatenate(hots, axis=1)
        hot_ref[g] = hot
        return total + dot(jnp.concatenate(lefts, axis=1), hot, NT)

    total = lax.fori_loop(0, rows // group, gather, jnp.zeros((12 * blocks, LANES), f32))
    for c in range(6):
        value = total[2 * c * blocks : (2 * c + 1) * blocks] + total[(2 * c + 1) * blocks : (2 * c + 2) * blocks]
        for a in range(blocks):
            motion_ref[c : c + 1, a * LANES : (a + 1) * LANES] = value[a : a + 1]
    wall = value
    wall_ref[...] = wall
    pressure = base_ref[...] + factor * wall
    left = []
    for c in range(3):
        normal = jnp.concatenate(
            [normals_ref[c : c + 1, a * LANES : (a + 1) * LANES] for a in range(blocks)], axis=0
        )
        left.extend(part.astype(f32) for part in split(normal * pressure))
    left = jnp.concatenate(left, axis=0).astype(bf16)

    def spread(g, carry):
        seen = dot(left, hot_ref[g], NN)
        for s in range(group):
            row = g * group + s
            at = slice(s * LANES, (s + 1) * LANES)
            weight = slots_ref[2, pl.ds(row, 1), :]
            mine = iota((blocks, LANES), 0).astype(f32) == slots_ref[0, pl.ds(row, 1), :]
            for c in range(3):
                both = (
                    seen[2 * c * blocks : (2 * c + 1) * blocks, at]
                    + seen[(2 * c + 1) * blocks : (2 * c + 2) * blocks, at]
                )
                load = weight * jnp.sum(jnp.where(mine, both, 0.0), axis=0, keepdims=True)
                out_ref[pl.ds(position(chunk_rows, 3, rows, c, row), 1), :] = load
        return carry

    lax.fori_loop(0, rows // group, spread, 0)


def force_kernel(chunk_rows, group, got_ref, asked_ref, base_ref, disp_ref, disp_out, vel_out, total_ref):
    rows = asked_ref.shape[0]
    nodes, width = disp_ref.shape[1], disp_ref.shape[2]
    half_nodes = nodes // 2
    total_ref[...] = jnp.zeros_like(total_ref)

    def step(g, carry):
        lefts, hots = [], []
        for s in range(group):
            row = g * group + s
            asked = asked_ref[pl.ds(row, 1), :]
            upper = asked // LANES - 1
            lower = asked % LANES
            second = upper >= half_nodes
            place = iota((half_nodes, LANES), 0) == jnp.where(second, upper - half_nodes, upper)
            hots.append(
                jnp.where(
                    iota((2 * width, LANES), 0) == jnp.where(second, lower + width, lower), 1.0, 0.0
                ).astype(bf16)
            )
            left = []
            for c in range(3):
                value = got_ref[pl.ds(position(chunk_rows, 3, rows, c, row), 1), :]
                for part in split(value):
                    left.append(jnp.where(place, part.astype(f32), 0.0))
            lefts.append(jnp.concatenate(left, axis=0).astype(bf16))
        total_ref[...] += dot(jnp.concatenate(lefts, axis=1), jnp.concatenate(hots, axis=1), NT)
        return carry

    lax.fori_loop(0, rows // group, step, 0)
    for c in range(3):
        for h in range(2):
            first = total_ref[2 * c * half_nodes : (2 * c + 1) * half_nodes, h * width : (h + 1) * width]
            second = total_ref[(2 * c + 1) * half_nodes : (2 * c + 2) * half_nodes, h * width : (h + 1) * width]
            at = slice(h * half_nodes, (h + 1) * half_nodes)
            vel_next = base_ref[c, at, :] + shell_step * (first + second)
            vel_out[c, at, :] = vel_next
            disp_out[c, at, :] = disp_ref[c, at, :] + shell_step * vel_next


def pack_kernel(
    disp_ref, fluid_ref, span_last, span_first, chord_last, chord_first, sems
):
    fields, cells_x, cells_y, _ = fluid_ref.shape
    nodes, width = disp_ref.shape[1], disp_ref.shape[2]
    copies = []

    def copy(source, target):
        one = pltpu.make_async_copy(source, target, sems.at[len(copies)])
        one.start()
        copies.append(one)

    for c in range(fields):
        copy(fluid_ref.at[c, pl.ds(cells_x - 3, 3)], span_last.at[pl.ds(3 * c, 3)])
        copy(fluid_ref.at[c, pl.ds(0, 3)], span_first.at[pl.ds(3 * c, 3)])
    for n, c in enumerate((0, 2)):
        copy(fluid_ref.at[c, :, pl.ds(cells_y - 8, 8)], chord_last.at[pl.ds(n * cells_x, cells_x)])
        copy(fluid_ref.at[c, :, pl.ds(0, 8)], chord_first.at[pl.ds(n * cells_x, cells_x)])
    for c in range(3):
        field = disp_ref[c]
        turned = field.T
        span_last[3 * fields, c : c + 1, :] = field[nodes - 1 :, :]
        span_first[3 * fields, c : c + 1, :] = field[:1, :]
        chord_last[2 * cells_x, c : c + 1, :] = turned[width - 1 :, :]
        chord_first[2 * cells_x, c : c + 1, :] = turned[:1, :]
    for one in copies:
        one.wait()


def coef(distance):
    size = jnp.abs(distance)
    value = jnp.where(size == 1, 45.0, jnp.where(size == 2, -9.0, jnp.where(size == 3, 1.0, 0.0)))
    return jnp.where(distance < 0, -value, value)


def flow_kernel(
    disp_ref, vel_ref, fluid_ref, before_x, after_x, before_y, after_y,
    next_ref, pressure_ref, surface_ref, shell_ref, wide, tall, normal, held, sems,
):
    fields, cells_x, cells_y, length = fluid_ref.shape
    nodes, width = disp_ref.shape[1], disp_ref.shape[2]
    copies = []

    def copy(source, target):
        one = pltpu.make_async_copy(source, target, sems.at[len(copies)])
        one.start()
        copies.append(one)

    for c in range(fields):
        copy(fluid_ref.at[c], wide.at[c, pl.ds(3, cells_x)])
    for n, c in enumerate((0, 2)):
        copy(fluid_ref.at[c], tall.at[n, :, pl.ds(8, cells_y)])
    for c in range(fields):
        wide[c, 0:3] = before_x[3 * c : 3 * c + 3]
        wide[c, 3 + cells_x : 6 + cells_x] = after_x[3 * c : 3 * c + 3]
    for n in range(2):
        tall[n, :, 0:8, :] = before_y[n * cells_x : (n + 1) * cells_x]
        tall[n, :, 8 + cells_y : 16 + cells_y, :] = after_y[n * cells_x : (n + 1) * cells_x]
    row = iota((nodes, width), 0)
    lane = iota((nodes, width), 1)
    for c in range(3):
        field = disp_ref[c]

        def column(plane, at):
            only = jnp.where(iota((8, width), 0) == c, plane, 0.0)
            place = jnp.where(iota((8, width), 1) == at, 1.0, 0.0).astype(bf16)
            high, low = split(only)
            return dot(high, place, TN) + dot(low, place, TN)

        left = column(before_y[2 * cells_x], 0)
        right = column(after_y[2 * cells_x], width - 1)
        above = jnp.where(row == 0, before_x[3 * fields, c : c + 1, :], pltpu.roll(field, 1, 0))
        below = jnp.where(
            row == nodes - 1, after_x[3 * fields, c : c + 1, :], pltpu.roll(field, nodes - 1, 0)
        )
        west = jnp.where(lane == 0, left, pltpu.roll(field, 1, 1))
        east = jnp.where(lane == width - 1, right, pltpu.roll(field, width - 1, 1))
        bending = above + below + west + east - 4.0 * field
        vel = vel_ref[c]
        shell_ref[c] = vel + shell_step * (stiffness * bending - damping * vel)
    source = iota((length, length), 0)
    target = iota((length, length), 1)
    inner = coef(source - target)
    ghost = jnp.where(source < 3, coef(-(source + 1 + target)), 0.0)
    for one in copies:
        one.wait()
    flat = cells_x * cells_y
    for n, field, table in ((0, 0, inner + ghost), (1, 3, inner - ghost)):
        table = table.astype(bf16)
        high, low = split(wide[field, 3 : 3 + cells_x].reshape(flat, length))
        total = dot(jnp.concatenate([high, low], axis=1), jnp.concatenate([table, table], axis=0), NN)
        normal[n] = (total * (1.0 / 60.0)).reshape(cells_x, cells_y, length)

    def central(window):
        return (
            0.75 * (window(1) - window(-1)) - 0.15 * (window(2) - window(-2))
        ) + (1.0 / 60.0) * (window(3) - window(-3))

    def plane(x):
        def along_x(field):
            return central(lambda offset: wide[field, x + 3 + offset])

        def along_y(slot):
            return central(lambda offset: tall[slot, x, 8 + offset : 8 + offset + cells_y, :])

        x_p = along_x(0)
        x_u = along_x(1)
        pressure_ref[x] = wide[0, x + 3] + time_step * (
            -flow_speed * x_p - (x_u + along_y(1) + normal[1, x])
        )
        held[0, x] = wide[1, x + 3] + time_step * (-flow_speed * x_u - x_p)
        held[1, x] = wide[2, x + 3] + time_step * (-flow_speed * along_x(2) - along_y(0))
        held[2, x] = wide[3, x + 3] + time_step * (-flow_speed * along_x(3) - normal[0, x])

    parts = 4
    size = cells_x // parts
    copies = []
    for part in range(parts):

        def planes(i, carry):
            plane(part * size + 2 * i)
            plane(part * size + 2 * i + 1)
            return carry

        lax.fori_loop(0, size // 2, planes, 0)
        at = pl.ds(part * size, size)
        one = pltpu.make_async_copy(held.at[:, at], next_ref.at[pl.ds(1, 3), at], sems.at[part])
        one.start()
        copies.append(one)
    lead = jnp.where((iota((8, length), 0) == 0) & (iota((8, length), 1) == 0), 1.0, 0.0).astype(bf16)
    blocks = surface_ref.shape[0]
    per = LANES // cells_y
    for b in range(blocks):
        high, low = split(pressure_ref[b * per : (b + 1) * per].reshape(LANES, length))
        found = dot(lead, high, NT) + dot(lead, low, NT)
        surface_ref[b : b + 1, :] = found[:1]
    for one in copies:
        one.wait()


def wall_kernel(wall_ref, pressure_ref, next_in, next_out):
    del next_in
    _, cells_x, cells_y, length = next_out.shape
    target = iota((8, length), 1)
    row = jnp.zeros((8, length), f32)
    for j in range(3):
        row = row + coef(-(j + 1 + target))
    row = jnp.where(iota((8, length), 0) == 0, row, 0.0).astype(bf16)
    per = LANES // cells_y
    for b in range(cells_x // per):
        wall = jnp.where(
            iota((8, LANES), 0) == 0, wall_ref[b : b + 1, :] * (-2.0 * time_step / 60.0), 0.0
        )
        high, low = split(wall)
        added = dot(high, row, TN) + dot(low, row, TN)
        at = slice(b * per, (b + 1) * per)
        next_out[0, at] = pressure_ref[at] + added.reshape(per, cells_y, length)


def exchange(value, devices, channels, chunk_rows, rows, capacity):
    if chunk_rows:
        shape = (devices, 1, channels * chunk_rows * LANES)
        got = lax.all_to_all(value.reshape(shape), AXES, split_axis=0, concat_axis=0, tiled=True)
        return got.reshape(channels * rows, LANES)
    value = value.reshape(channels, devices, capacity).transpose(1, 0, 2)
    got = lax.all_to_all(value, AXES, split_axis=0, concat_axis=0, tiled=True)
    return got.transpose(1, 0, 2).reshape(channels * rows, LANES)


def body(fluid_state, shell_disp, shell_vel, owners, node_local, rbf_weight, normals):
    span_count = lax.axis_size("span")
    chord_count = lax.axis_size("chord")
    devices = span_count * chord_count
    points, stencil = owners.shape
    capacity = max(2, (2 * points * stencil + devices - 1) // devices)
    rows = devices * capacity // LANES
    chunk_rows = capacity // LANES if capacity % LANES == 0 else 0
    blocks = points // LANES
    fields, cells_x, cells_y, length = fluid_state.shape
    _, nodes, width = shell_disp.shape
    sds = jax.ShapeDtypeStruct
    vmem = pl.BlockSpec(memory_space=pltpu.VMEM)
    hbm = pl.BlockSpec(memory_space=pl.ANY)

    near_out = pltpu.VMEM
    requests, dest = call(
        functools.partial(route_kernel, devices, capacity),
        [near_out((rows, LANES), i32), near_out((stencil, points), i32)],
        owners.T,
        node_local.T,
    )
    asked = exchange(requests, devices, 1, chunk_rows, rows, capacity)

    slots = call(
        slots_kernel,
        near_out((3, rows, LANES), f32),
        dest,
        rbf_weight.T,
        held=(0,),
        flops=200_000_000,
    )
    table = call(table_kernel, near_out((6 * width, 2 * nodes), bf16), shell_disp, shell_vel)

    span_shape = near_out((3 * fields + 1, cells_y, length), f32)
    chord_shape = near_out((2 * cells_x + 1, 8, length), f32)
    span_last, span_first, chord_last, chord_first = call(
        pack_kernel,
        [span_shape, span_shape, chord_shape, chord_shape],
        shell_disp,
        fluid_state,
        in_specs=[vmem, hbm],
        scratch_shapes=[pltpu.SemaphoreType.DMA((2 * fields + 4,))],
    )

    def shifted(last, leading, axis, size):
        up = [(i, i + 1) for i in range(size - 1)]
        down = [(i + 1, i) for i in range(size - 1)]
        return lax.ppermute(last, axis, up), lax.ppermute(leading, axis, down)

    before_x, after_x = shifted(span_last, span_first, "span", span_count)
    before_y, after_y = shifted(chord_last, chord_first, "chord", chord_count)

    flow_next, pressure, surface, shell_base = call(
        flow_kernel,
        [
            sds(fluid_state.shape, f32),
            near_out((cells_x, cells_y, length), f32),
            near_out((blocks, LANES), f32),
            near_out(shell_disp.shape, f32),
        ],
        shell_disp,
        shell_vel,
        fluid_state,
        before_x,
        after_x,
        before_y,
        after_y,
        flops=300_000_000,
        held=(0, 1, 3, 4, 5, 6),
        in_specs=[vmem, vmem, hbm, vmem, vmem, vmem, vmem],
        out_specs=[hbm, vmem, vmem, vmem],
        scratch_shapes=[
            pltpu.VMEM((fields, cells_x + 6, cells_y, length), f32),
            pltpu.VMEM((2, cells_x, cells_y + 16, length), f32),
            pltpu.VMEM((2, cells_x, cells_y, length), f32),
            pltpu.VMEM((3, cells_x, cells_y, length), f32),
            pltpu.SemaphoreType.DMA((fields + 2,)),
        ],
    )

    picked = call(
        functools.partial(fetch_kernel, chunk_rows, 4),
        near_out((6 * rows, LANES), f32),
        asked,
        table,
        held=(0, 1),
        flops=3_000_000_000,
    )
    replies = exchange(picked, devices, 6, chunk_rows, rows, capacity)

    wall_first = 2.0 * (-45.0 + 9.0 - 1.0) / 60.0
    interface_motion, wall, loads = call(
        functools.partial(meet_kernel, chunk_rows, 8, -time_step * wall_first),
        [
            sds((6, points), f32),
            near_out((blocks, LANES), f32),
            near_out((3 * rows, LANES), f32),
        ],
        replies,
        slots,
        surface,
        normals,
        held=(0, 1, 2, 3),
        flops=300_000_000,
        scratch_shapes=[pltpu.VMEM((rows // 8, LANES, 8 * LANES), bf16)],
    )
    arrived = exchange(loads, devices, 3, chunk_rows, rows, capacity)

    block = pl.BlockSpec((1, cells_x, cells_y, length), lambda i: (0, 0, 0, 0))
    fluid_next = call(
        wall_kernel,
        sds(fluid_state.shape, f32),
        wall,
        pressure,
        flow_next,
        flops=100_000_000,
        held=(0, 1),
        grid=(1,),
        in_specs=[vmem, vmem, hbm],
        out_specs=block,
        input_output_aliases={2: 0},
    )

    disp_next, vel_next = call(
        functools.partial(force_kernel, chunk_rows, 8),
        [sds(shell_disp.shape, f32), sds(shell_vel.shape, f32)],
        arrived,
        asked,
        shell_base,
        shell_disp,
        held=(0, 1, 2, 3),
        flops=3_000_000_000,
        scratch_shapes=[pltpu.VMEM((3 * nodes, 2 * width), f32)],
    )
    return (fluid_next, interface_motion, disp_next, vel_next)


def solution(mesh):
    placed = (
        P(None, "span", "chord", None),
        P(None, "span", "chord"),
        P(None, "span", "chord"),
        P(AXES, None),
        P(AXES, None),
        P(AXES, None),
        P(None, AXES),
    )

    return jax.shard_map(
        body,
        mesh=mesh,
        in_specs=placed,
        out_specs=(
            P(None, "span", "chord", None),
            P(None, AXES),
            P(None, "span", "chord"),
            P(None, "span", "chord"),
        ),
        check_vma=False,
    )
```

```python
import functools

import jax
import jax.numpy as jnp
from jax import lax
from jax.experimental import pallas as pl
from jax.experimental.pallas import tpu as pltpu
from jax.sharding import PartitionSpec as P


flow_speed = 0.5
time_step = 0.4
stiffness = 0.5
damping = 0.2
shell_step = 0.3

AXES = ("span", "chord")
LANES = 128
f32 = jnp.float32
bf16 = jnp.bfloat16
i32 = jnp.int32
NT = (((1,), (1,)), ((), ()))
TN = (((0,), (0,)), ((), ()))
NN = (((1,), (0,)), ((), ()))


def dot(a, b, dims, precision=None):
    return lax.dot_general(a, b, dims, precision=precision, preferred_element_type=f32)


def iota(shape, dim):
    return lax.broadcasted_iota(i32, shape, dim)


def split(value):
    high = value.astype(bf16)
    low = (value - high.astype(f32)).astype(bf16)
    return high, low


def near(value):
    return pltpu.with_memory_space_constraint(value, pltpu.VMEM)


def call(kernel, outs, *args, flops=1_000_000, held=(), **kw):
    single = not isinstance(outs, (list, tuple))
    space = pl.BlockSpec(memory_space=pltpu.VMEM)
    kw.setdefault("in_specs", [space] * len(args))
    args = [near(a) if n in held else a for n, a in enumerate(args)]
    kw.setdefault("out_specs", space if single else [space] * len(outs))
    nbytes = sum(a.size * a.dtype.itemsize for a in args)
    return pl.pallas_call(
        kernel,
        out_shape=outs,
        cost_estimate=pl.CostEstimate(flops=flops, transcendentals=0, bytes_accessed=nbytes),
        **kw,
    )(*args)


def route_kernel(
    devices, capacity, own_ref, node_ref, disp_hbm, vel_hbm, fluid_ref,
    req_hbm, dest_ref, table_ref, span_a, span_b, chord_a, chord_b,
    req_ref, disp_ref, vel_ref, sems,
):
    fields, cells_x, cells_y, _ = fluid_ref.shape
    copies = []

    def copy(source, target):
        one = pltpu.make_async_copy(source, target, sems.at[len(copies)])
        one.start()
        copies.append(one)

    copy(disp_hbm, disp_ref)
    copy(vel_hbm, vel_ref)
    odd_x = lax.axis_index("span") % 2
    odd_y = lax.axis_index("chord") % 2
    for c in range(fields):
        copy(fluid_ref.at[c, pl.ds((1 - odd_x) * (cells_x - 3), 3)], span_a.at[pl.ds(3 * c, 3)])
        copy(fluid_ref.at[c, pl.ds(odd_x * (cells_x - 3), 3)], span_b.at[pl.ds(3 * c, 3)])
    for n, c in enumerate((0, 2)):
        first = pl.multiple_of((1 - odd_y) * (cells_y - 8), 8)
        copy(fluid_ref.at[c, :, pl.ds(first, 8)], chord_a.at[pl.ds(n * cells_x, cells_x)])
        first = pl.multiple_of(odd_y * (cells_y - 8), 8)
        copy(fluid_ref.at[c, :, pl.ds(first, 8)], chord_b.at[pl.ds(n * cells_x, cells_x)])
    stencil, points = own_ref.shape
    blocks = points // LANES
    rows = req_ref.shape[0]
    member = []
    for b in range(blocks):
        ids = iota((devices, LANES), 0)
        hit = jnp.zeros((devices, LANES), f32)
        for k in range(stencil):
            hit = jnp.where(own_ref[k : k + 1, b * LANES : (b + 1) * LANES] == ids, 1.0, hit)
        member.append(hit)
    stacked = jnp.concatenate(member, axis=0).astype(bf16)
    source = iota((LANES, 2 * LANES), 0)
    target = iota((LANES, 2 * LANES), 1)
    table = jnp.where((source < target) | (target >= LANES), 1.0, 0.0).astype(bf16)
    counted = dot(stacked, table, NN)
    offset = jnp.zeros((devices, LANES), f32)
    for b in range(blocks):
        part = counted[b * devices : (b + 1) * devices]
        rank = part[:, :LANES] + offset
        offset = offset + part[:, LANES:]
        ids = iota((devices, LANES), 0)
        for k in range(stencil):
            own = own_ref[k : k + 1, b * LANES : (b + 1) * LANES]
            mine = jnp.sum(jnp.where(own == ids, rank, 0.0), axis=0, keepdims=True)
            dest_ref[k : k + 1, b * LANES : (b + 1) * LANES] = own * capacity + mine.astype(i32)
    total = jnp.zeros((2 * rows, LANES), f32)
    for k in range(stencil):
        dest = dest_ref[k : k + 1, :]
        node = node_ref[k : k + 1, :]
        place = iota((rows, points), 0) == dest // LANES
        upper = (node // LANES + 1).astype(f32)
        lower = (node % LANES).astype(f32)
        left = jnp.concatenate(
            [jnp.where(place, upper, 0.0), jnp.where(place, lower, 0.0)], axis=0
        ).astype(bf16)
        right = jnp.where(iota((LANES, points), 0) == dest % LANES, 1.0, 0.0).astype(bf16)
        total = total + dot(left, right, NT)
    req_ref[...] = (total[:rows] * LANES + total[rows:]).astype(i32)
    copy(req_ref, req_hbm)
    copies[0].wait()
    copies[1].wait()
    nodes, width = disp_ref.shape[1], disp_ref.shape[2]
    half = width // 2
    for c in range(6):
        field = disp_ref[c] if c < 3 else vel_ref[c - 3]
        turned = field.T
        if c < 3:
            ends = (field[nodes - 1 :, :], field[:1, :])
            span_a[3 * fields, c : c + 1, :] = jnp.where(odd_x == 0, *ends)
            span_b[3 * fields, c : c + 1, :] = jnp.where(odd_x == 1, *ends)
            ends = (turned[width - 1 :, :], turned[:1, :])
            chord_a[2 * cells_x, c : c + 1, :] = jnp.where(odd_y == 0, *ends)
            chord_b[2 * cells_x, c : c + 1, :] = jnp.where(odd_y == 1, *ends)
        for n, part in enumerate(split(turned)):
            for h in range(2):
                first = (6 * n + c) * half
                table_ref[first : first + half, h * nodes : (h + 1) * nodes] = part[
                    h * half : (h + 1) * half
                ]
    for one in copies[2:]:
        one.wait()


def slots_kernel(dest_ref, weight_ref, slots_ref):
    stencil, points = dest_ref.shape
    rows = slots_ref.shape[1]
    total = jnp.zeros((4 * rows, LANES), f32)
    point = iota((1, points), 1)
    point_a = (point // LANES).astype(f32)
    point_b = (point % LANES).astype(f32)
    for k in range(stencil):
        dest = dest_ref[k : k + 1, :]
        high, low = split(weight_ref[k : k + 1, :])
        place = iota((rows, points), 0) == dest // LANES
        parts = [point_a, point_b, high.astype(f32), low.astype(f32)]
        left = jnp.concatenate([jnp.where(place, part, 0.0) for part in parts], axis=0)
        right = jnp.where(iota((LANES, points), 0) == dest % LANES, 1.0, 0.0).astype(bf16)
        total = total + dot(left.astype(bf16), right, NT)
    slots_ref[0] = total[:rows]
    slots_ref[1] = total[rows : 2 * rows]
    slots_ref[2] = total[2 * rows : 3 * rows] + total[3 * rows :]


def pair(ref, first, start=None):
    if start is None:
        return jnp.concatenate([ref[pl.ds(first, 1), :], ref[pl.ds(first + 1, 1), :]], axis=1)
    return jnp.concatenate(
        [ref[start, pl.ds(first, 1), :], ref[start, pl.ds(first + 1, 1), :]], axis=1
    )


def position(chunk_rows, channels, rows, channel, row):
    if chunk_rows:
        return (row // chunk_rows) * (channels * chunk_rows) + channel * chunk_rows + row % chunk_rows
    return channel * rows + row


def fetch_kernel(chunk_rows, group, asked_ref, table_ref, out_ref):
    rows = asked_ref.shape[0]
    half = table_ref.shape[0] // 12
    double = table_ref.shape[1]
    nodes = double // 2

    def step(g, carry):
        for s in range(group):
            t = g * group + s
            asked = pair(asked_ref, 2 * t)
            lower = asked % LANES
            upper = asked // LANES - 1
            second = lower >= half
            at = jnp.where(upper < 0, -1, jnp.where(second, upper + nodes, upper))
            hot = jnp.where(iota((double, 2 * LANES), 0) == at, 1.0, 0.0).astype(bf16)
            picked = dot(table_ref[...], hot, NN)
            picked = picked[: 6 * half] + picked[6 * half :]
            keep = iota((half, 2 * LANES), 0) == jnp.where(second, lower - half, lower)
            for c in range(6):
                found = jnp.sum(
                    jnp.where(keep, picked[c * half : (c + 1) * half], 0.0), axis=0, keepdims=True
                )
                for h in range(2):
                    to = position(chunk_rows, 6, rows, c, 2 * t + h)
                    out_ref[pl.ds(to, 1), :] = found[:, h * LANES : (h + 1) * LANES]
        return carry

    lax.fori_loop(0, rows // (2 * group), step, 0)


def meet_kernel(
    chunk_rows, group, factor, got_ref, slots_ref, base_ref, normals_ref, motion_ref, wall_ref, out_ref,
    hot_ref,
):
    rows = slots_ref.shape[1]
    blocks = base_ref.shape[0]

    def gather(g, total):
        lefts, hots = [], []
        for s in range(group):
            row = g * group + s
            weight = slots_ref[2, pl.ds(row, 1), :]
            mine = iota((blocks, LANES), 0).astype(f32) == slots_ref[0, pl.ds(row, 1), :]
            hot = jnp.where(
                iota((LANES, LANES), 0).astype(f32) == slots_ref[1, pl.ds(row, 1), :], 1.0, 0.0
            ).astype(bf16)
            left = []
            for c in range(6):
                value = got_ref[pl.ds(position(chunk_rows, 6, rows, c, row), 1), :]
                for part in split(value * weight):
                    left.append(jnp.where(mine, part.astype(f32), 0.0))
            lefts.append(jnp.concatenate(left, axis=0).astype(bf16))
            hots.append(hot)
        hot = jnp.concatenate(hots, axis=1)
        hot_ref[g] = hot
        return total + dot(jnp.concatenate(lefts, axis=1), hot, NT)

    total = lax.fori_loop(0, rows // group, gather, jnp.zeros((12 * blocks, LANES), f32))
    for c in range(6):
        value = total[2 * c * blocks : (2 * c + 1) * blocks] + total[(2 * c + 1) * blocks : (2 * c + 2) * blocks]
        for a in range(blocks):
            motion_ref[c : c + 1, a * LANES : (a + 1) * LANES] = value[a : a + 1]
    wall = value
    wall_ref[...] = wall
    pressure = base_ref[...] + factor * wall
    left = []
    for c in range(3):
        normal = jnp.concatenate(
            [normals_ref[c : c + 1, a * LANES : (a + 1) * LANES] for a in range(blocks)], axis=0
        )
        left.extend(part.astype(f32) for part in split(normal * pressure))
    left = jnp.concatenate(left, axis=0).astype(bf16)

    def spread(g, carry):
        seen = dot(left, hot_ref[g], NN)
        for s in range(group):
            row = g * group + s
            at = slice(s * LANES, (s + 1) * LANES)
            weight = slots_ref[2, pl.ds(row, 1), :]
            mine = iota((blocks, LANES), 0).astype(f32) == slots_ref[0, pl.ds(row, 1), :]
            for c in range(3):
                both = (
                    seen[2 * c * blocks : (2 * c + 1) * blocks, at]
                    + seen[(2 * c + 1) * blocks : (2 * c + 2) * blocks, at]
                )
                load = weight * jnp.sum(jnp.where(mine, both, 0.0), axis=0, keepdims=True)
                out_ref[pl.ds(position(chunk_rows, 3, rows, c, row), 1), :] = load
        return carry

    lax.fori_loop(0, rows // group, spread, 0)


def force_kernel(chunk_rows, group, got_ref, asked_ref, base_ref, disp_ref, disp_out, vel_out, total_ref):
    rows = asked_ref.shape[0]
    nodes, width = disp_ref.shape[1], disp_ref.shape[2]
    half_nodes = nodes // 2
    total_ref[...] = jnp.zeros_like(total_ref)

    def step(g, carry):
        lefts, hots = [], []
        for s in range(group):
            row = g * group + s
            asked = asked_ref[pl.ds(row, 1), :]
            upper = asked // LANES - 1
            lower = asked % LANES
            second = upper >= half_nodes
            place = iota((half_nodes, LANES), 0) == jnp.where(second, upper - half_nodes, upper)
            hots.append(
                jnp.where(
                    iota((2 * width, LANES), 0) == jnp.where(second, lower + width, lower), 1.0, 0.0
                ).astype(bf16)
            )
            left = []
            for c in range(3):
                value = got_ref[pl.ds(position(chunk_rows, 3, rows, c, row), 1), :]
                for part in split(value):
                    left.append(jnp.where(place, part.astype(f32), 0.0))
            lefts.append(jnp.concatenate(left, axis=0).astype(bf16))
        total_ref[...] += dot(jnp.concatenate(lefts, axis=1), jnp.concatenate(hots, axis=1), NT)
        return carry

    lax.fori_loop(0, rows // group, step, 0)
    for c in range(3):
        for h in range(2):
            first = total_ref[2 * c * half_nodes : (2 * c + 1) * half_nodes, h * width : (h + 1) * width]
            second = total_ref[(2 * c + 1) * half_nodes : (2 * c + 2) * half_nodes, h * width : (h + 1) * width]
            at = slice(h * half_nodes, (h + 1) * half_nodes)
            vel_next = base_ref[c, at, :] + shell_step * (first + second)
            vel_out[c, at, :] = vel_next
            disp_out[c, at, :] = disp_ref[c, at, :] + shell_step * vel_next


def coef(distance):
    size = jnp.abs(distance)
    value = jnp.where(size == 1, 45.0, jnp.where(size == 2, -9.0, jnp.where(size == 3, 1.0, 0.0)))
    return jnp.where(distance < 0, -value, value)


def flow_kernel(
    disp_ref, vel_ref, fluid_ref, got_xa, got_xb, got_ya, got_yb,
    next_ref, pressure_ref, surface_ref, shell_ref, wide, tall, normal, held, sems,
):
    fields, cells_x, cells_y, length = fluid_ref.shape
    nodes, width = disp_ref.shape[1], disp_ref.shape[2]
    copies = []

    def copy(source, target):
        one = pltpu.make_async_copy(source, target, sems.at[len(copies)])
        one.start()
        copies.append(one)

    for c in range(fields):
        copy(fluid_ref.at[c], wide.at[c, pl.ds(3, cells_x)])
    for n, c in enumerate((0, 2)):
        copy(fluid_ref.at[c], tall.at[n, :, pl.ds(8, cells_y)])
    odd_x = lax.axis_index("span") % 2
    odd_y = lax.axis_index("chord") % 2
    for got, side in ((got_xa, 1 - odd_x), (got_xb, odd_x)):
        for c in range(fields):
            wide[c, pl.ds(side * (cells_x + 3), 3)] = got[3 * c : 3 * c + 3]
    for got, side in ((got_ya, 1 - odd_y), (got_yb, odd_y)):
        first = pl.multiple_of(side * (cells_y + 8), 8)
        for n in range(2):
            tall[n, :, pl.ds(first, 8), :] = got[n * cells_x : (n + 1) * cells_x]
    ends_x = (got_xa[3 * fields, :8, :], got_xb[3 * fields, :8, :])
    before_x, after_x = jnp.where(odd_x == 1, *ends_x), jnp.where(odd_x == 0, *ends_x)
    ends_y = (got_ya[2 * cells_x], got_yb[2 * cells_x])
    before_y, after_y = jnp.where(odd_y == 1, *ends_y), jnp.where(odd_y == 0, *ends_y)
    row = iota((nodes, width), 0)
    lane = iota((nodes, width), 1)
    for c in range(3):
        field = disp_ref[c]

        def column(plane, at):
            only = jnp.where(iota((8, width), 0) == c, plane, 0.0)
            place = jnp.where(iota((8, width), 1) == at, 1.0, 0.0).astype(bf16)
            high, low = split(only)
            return dot(high, place, TN) + dot(low, place, TN)

        left = column(before_y, 0)
        right = column(after_y, width - 1)
        above = jnp.where(row == 0, before_x[c : c + 1, :], pltpu.roll(field, 1, 0))
        below = jnp.where(
            row == nodes - 1, after_x[c : c + 1, :], pltpu.roll(field, nodes - 1, 0)
        )
        west = jnp.where(lane == 0, left, pltpu.roll(field, 1, 1))
        east = jnp.where(lane == width - 1, right, pltpu.roll(field, width - 1, 1))
        bending = above + below + west + east - 4.0 * field
        vel = vel_ref[c]
        shell_ref[c] = vel + shell_step * (stiffness * bending - damping * vel)
    source = iota((length, length), 0)
    target = iota((length, length), 1)
    inner = coef(source - target)
    ghost = jnp.where(source < 3, coef(-(source + 1 + target)), 0.0)
    for one in copies:
        one.wait()
    flat = cells_x * cells_y
    for n, field, table in ((0, 0, inner + ghost), (1, 3, inner - ghost)):
        table = table.astype(bf16)
        high, low = split(wide[field, 3 : 3 + cells_x].reshape(flat, length))
        total = dot(jnp.concatenate([high, low], axis=1), jnp.concatenate([table, table], axis=0), NN)
        normal[n] = (total * (1.0 / 60.0)).reshape(cells_x, cells_y, length)

    def central(window):
        return (
            0.75 * (window(1) - window(-1)) - 0.15 * (window(2) - window(-2))
        ) + (1.0 / 60.0) * (window(3) - window(-3))

    def plane(x):
        def along_x(field):
            return central(lambda offset: wide[field, x + 3 + offset])

        def along_y(slot):
            return central(lambda offset: tall[slot, x, 8 + offset : 8 + offset + cells_y, :])

        x_p = along_x(0)
        x_u = along_x(1)
        pressure_ref[x] = wide[0, x + 3] + time_step * (
            -flow_speed * x_p - (x_u + along_y(1) + normal[1, x])
        )
        held[0, x] = wide[1, x + 3] + time_step * (-flow_speed * x_u - x_p)
        held[1, x] = wide[2, x + 3] + time_step * (-flow_speed * along_x(2) - along_y(0))
        held[2, x] = wide[3, x + 3] + time_step * (-flow_speed * along_x(3) - normal[0, x])

    parts = 4
    size = cells_x // parts
    copies = []
    for part in range(parts):

        def planes(i, carry):
            plane(part * size + 2 * i)
            plane(part * size + 2 * i + 1)
            return carry

        lax.fori_loop(0, size // 2, planes, 0)
        at = pl.ds(part * size, size)
        one = pltpu.make_async_copy(held.at[:, at], next_ref.at[pl.ds(1, 3), at], sems.at[part])
        one.start()
        copies.append(one)
    lead = jnp.where((iota((8, length), 0) == 0) & (iota((8, length), 1) == 0), 1.0, 0.0).astype(bf16)
    blocks = surface_ref.shape[0]
    per = LANES // cells_y
    for b in range(blocks):
        high, low = split(pressure_ref[b * per : (b + 1) * per].reshape(LANES, length))
        found = dot(lead, high, NT) + dot(lead, low, NT)
        surface_ref[b : b + 1, :] = found[:1]
    for one in copies:
        one.wait()


def wall_kernel(wall_ref, pressure_ref, next_in, next_out):
    del next_in
    _, cells_x, cells_y, length = next_out.shape
    target = iota((8, length), 1)
    row = jnp.zeros((8, length), f32)
    for j in range(3):
        row = row + coef(-(j + 1 + target))
    row = jnp.where(iota((8, length), 0) == 0, row, 0.0).astype(bf16)
    per = LANES // cells_y
    for b in range(cells_x // per):
        wall = jnp.where(
            iota((8, LANES), 0) == 0, wall_ref[b : b + 1, :] * (-2.0 * time_step / 60.0), 0.0
        )
        high, low = split(wall)
        added = dot(high, row, TN) + dot(low, row, TN)
        at = slice(b * per, (b + 1) * per)
        next_out[0, at] = pressure_ref[at] + added.reshape(per, cells_y, length)


def exchange(value, devices, channels, chunk_rows, rows, capacity):
    if chunk_rows:
        shape = (devices, 1, channels * chunk_rows * LANES)
        got = lax.all_to_all(value.reshape(shape), AXES, split_axis=0, concat_axis=0, tiled=True)
        return got.reshape(channels * rows, LANES)
    value = value.reshape(channels, devices, capacity).transpose(1, 0, 2)
    got = lax.all_to_all(value, AXES, split_axis=0, concat_axis=0, tiled=True)
    return got.transpose(1, 0, 2).reshape(channels * rows, LANES)


def body(fluid_state, shell_disp, shell_vel, owners, node_local, rbf_weight, normals):
    span_count = lax.axis_size("span")
    chord_count = lax.axis_size("chord")
    devices = span_count * chord_count
    points, stencil = owners.shape
    capacity = max(2, (2 * points * stencil + devices - 1) // devices)
    rows = devices * capacity // LANES
    chunk_rows = capacity // LANES if capacity % LANES == 0 else 0
    blocks = points // LANES
    fields, cells_x, cells_y, length = fluid_state.shape
    _, nodes, width = shell_disp.shape
    sds = jax.ShapeDtypeStruct
    vmem = pl.BlockSpec(memory_space=pltpu.VMEM)
    hbm = pl.BlockSpec(memory_space=pl.ANY)

    near_out = pltpu.VMEM
    span_shape = near_out((3 * fields + 1, cells_y, length), f32)
    chord_shape = near_out((2 * cells_x + 1, 8, length), f32)
    requests, dest, table, span_a, span_b, chord_a, chord_b = call(
        functools.partial(route_kernel, devices, capacity),
        [
            sds((rows, LANES), i32),
            near_out((stencil, points), i32),
            near_out((6 * width, 2 * nodes), bf16),
            span_shape,
            span_shape,
            chord_shape,
            chord_shape,
        ],
        owners.T,
        node_local.T,
        shell_disp,
        shell_vel,
        fluid_state,
        flops=100_000_000,
        in_specs=[vmem, vmem, hbm, hbm, hbm],
        out_specs=[hbm] + [vmem] * 6,
        scratch_shapes=[
            pltpu.VMEM((rows, LANES), i32),
            pltpu.VMEM(shell_disp.shape, f32),
            pltpu.VMEM(shell_vel.shape, f32),
            pltpu.SemaphoreType.DMA((2 * fields + 7,)),
        ],
    )

    def swapped(one, two, axis, size):
        even = [pair for i in range(0, size - 1, 2) for pair in ((i, i + 1), (i + 1, i))]
        odd = [pair for i in range(1, size - 1, 2) for pair in ((i, i + 1), (i + 1, i))]
        first = lax.ppermute(one, axis, even)
        return first, lax.ppermute(two, axis, odd)

    got_xa, got_xb = swapped(span_a, span_b, "span", span_count)
    got_ya, got_yb = swapped(chord_a, chord_b, "chord", chord_count)

    asked = exchange(requests, devices, 1, chunk_rows, rows, capacity)

    slots = call(
        slots_kernel,
        near_out((3, rows, LANES), f32),
        dest,
        rbf_weight.T,
        held=(0,),
        flops=200_000_000,
    )
    flow_next, pressure, surface, shell_base = call(
        flow_kernel,
        [
            sds(fluid_state.shape, f32),
            near_out((cells_x, cells_y, length), f32),
            near_out((blocks, LANES), f32),
            near_out(shell_disp.shape, f32),
        ],
        shell_disp,
        shell_vel,
        fluid_state,
        got_xa,
        got_xb,
        got_ya,
        got_yb,
        flops=300_000_000,
        held=(0, 1, 3, 4, 5, 6),
        in_specs=[vmem, vmem, hbm, vmem, vmem, vmem, vmem],
        out_specs=[hbm, vmem, vmem, vmem],
        scratch_shapes=[
            pltpu.VMEM((fields, cells_x + 6, cells_y, length), f32),
            pltpu.VMEM((2, cells_x, cells_y + 16, length), f32),
            pltpu.VMEM((2, cells_x, cells_y, length), f32),
            pltpu.VMEM((3, cells_x, cells_y, length), f32),
            pltpu.SemaphoreType.DMA((fields + 2,)),
        ],
    )

    picked = call(
        functools.partial(fetch_kernel, chunk_rows, 32),
        near_out((6 * rows, LANES), f32),
        asked,
        table,
        held=(0, 1),
        flops=3_000_000_000,
    )
    replies = exchange(picked, devices, 6, chunk_rows, rows, capacity)

    wall_first = 2.0 * (-45.0 + 9.0 - 1.0) / 60.0
    interface_motion, wall, loads = call(
        functools.partial(meet_kernel, chunk_rows, 32, -time_step * wall_first),
        [
            sds((6, points), f32),
            near_out((blocks, LANES), f32),
            near_out((3 * rows, LANES), f32),
        ],
        replies,
        slots,
        surface,
        normals,
        held=(0, 1, 2, 3),
        flops=300_000_000,
        scratch_shapes=[pltpu.VMEM((rows // 32, LANES, 32 * LANES), bf16)],
    )
    arrived = exchange(loads, devices, 3, chunk_rows, rows, capacity)

    block = pl.BlockSpec((1, cells_x, cells_y, length), lambda i: (0, 0, 0, 0))
    fluid_next = call(
        wall_kernel,
        sds(fluid_state.shape, f32),
        wall,
        pressure,
        flow_next,
        flops=100_000_000,
        held=(0, 1),
        grid=(1,),
        in_specs=[vmem, vmem, hbm],
        out_specs=block,
        input_output_aliases={2: 0},
    )

    disp_next, vel_next = call(
        functools.partial(force_kernel, chunk_rows, 64),
        [sds(shell_disp.shape, f32), sds(shell_vel.shape, f32)],
        arrived,
        asked,
        shell_base,
        shell_disp,
        held=(0, 1, 2, 3),
        flops=3_000_000_000,
        scratch_shapes=[pltpu.VMEM((3 * nodes, 2 * width), f32)],
    )
    return (fluid_next, interface_motion, disp_next, vel_next)


def solution(mesh):
    placed = (
        P(None, "span", "chord", None),
        P(None, "span", "chord"),
        P(None, "span", "chord"),
        P(AXES, None),
        P(AXES, None),
        P(AXES, None),
        P(None, AXES),
    )

    return jax.shard_map(
        body,
        mesh=mesh,
        in_specs=placed,
        out_specs=(
            P(None, "span", "chord", None),
            P(None, AXES),
            P(None, "span", "chord"),
            P(None, "span", "chord"),
        ),
        check_vma=False,
    )
```

```python
import functools

import jax
import jax.numpy as jnp
from jax import lax
from jax.experimental import pallas as pl
from jax.experimental.pallas import tpu as pltpu
from jax.sharding import PartitionSpec as P


flow_speed = 0.5
time_step = 0.4
stiffness = 0.5
damping = 0.2
shell_step = 0.3

AXES = ("span", "chord")
LANES = 128
f32 = jnp.float32
bf16 = jnp.bfloat16
i32 = jnp.int32
NT = (((1,), (1,)), ((), ()))
TN = (((0,), (0,)), ((), ()))
NN = (((1,), (0,)), ((), ()))


def dot(a, b, dims, precision=None):
    return lax.dot_general(a, b, dims, precision=precision, preferred_element_type=f32)


def iota(shape, dim):
    return lax.broadcasted_iota(i32, shape, dim)


def split(value):
    high = value.astype(bf16)
    low = (value - high.astype(f32)).astype(bf16)
    return high, low


def near(value):
    return pltpu.with_memory_space_constraint(value, pltpu.VMEM)


def call(kernel, outs, *args, flops=1_000_000, held=(), **kw):
    single = not isinstance(outs, (list, tuple))
    space = pl.BlockSpec(memory_space=pltpu.VMEM)
    kw.setdefault("in_specs", [space] * len(args))
    args = [near(a) if n in held else a for n, a in enumerate(args)]
    kw.setdefault("out_specs", space if single else [space] * len(outs))
    nbytes = sum(a.size * a.dtype.itemsize for a in args)
    return pl.pallas_call(
        kernel,
        out_shape=outs,
        cost_estimate=pl.CostEstimate(flops=flops, transcendentals=0, bytes_accessed=nbytes),
        **kw,
    )(*args)


def route_kernel(
    devices, capacity, own_ref, node_ref, disp_hbm, vel_hbm, fluid_ref,
    req_hbm, dest_ref, table_ref, span_a, span_b, chord_a, chord_b,
    req_ref, disp_ref, vel_ref, sems,
):
    fields, cells_x, cells_y, _ = fluid_ref.shape
    copies = []

    def copy(source, target):
        one = pltpu.make_async_copy(source, target, sems.at[len(copies)])
        one.start()
        copies.append(one)

    copy(disp_hbm, disp_ref)
    copy(vel_hbm, vel_ref)
    odd_x = lax.axis_index("span") % 2
    odd_y = lax.axis_index("chord") % 2
    for c in range(fields):
        copy(fluid_ref.at[c, pl.ds((1 - odd_x) * (cells_x - 3), 3)], span_a.at[pl.ds(3 * c, 3)])
        copy(fluid_ref.at[c, pl.ds(odd_x * (cells_x - 3), 3)], span_b.at[pl.ds(3 * c, 3)])
    for n, c in enumerate((0, 2)):
        first = pl.multiple_of((1 - odd_y) * (cells_y - 8), 8)
        copy(fluid_ref.at[c, :, pl.ds(first, 8)], chord_a.at[pl.ds(n * cells_x, cells_x)])
        first = pl.multiple_of(odd_y * (cells_y - 8), 8)
        copy(fluid_ref.at[c, :, pl.ds(first, 8)], chord_b.at[pl.ds(n * cells_x, cells_x)])
    stencil, points = own_ref.shape
    blocks = points // LANES
    rows = req_ref.shape[0]
    member = []
    for b in range(blocks):
        ids = iota((devices, LANES), 0)
        hit = jnp.zeros((devices, LANES), f32)
        for k in range(stencil):
            hit = jnp.where(own_ref[k : k + 1, b * LANES : (b + 1) * LANES] == ids, 1.0, hit)
        member.append(hit)
    stacked = jnp.concatenate(member, axis=0).astype(bf16)
    source = iota((LANES, 2 * LANES), 0)
    target = iota((LANES, 2 * LANES), 1)
    table = jnp.where((source < target) | (target >= LANES), 1.0, 0.0).astype(bf16)
    counted = dot(stacked, table, NN)
    offset = jnp.zeros((devices, LANES), f32)
    for b in range(blocks):
        part = counted[b * devices : (b + 1) * devices]
        rank = part[:, :LANES] + offset
        offset = offset + part[:, LANES:]
        ids = iota((devices, LANES), 0)
        for k in range(stencil):
            own = own_ref[k : k + 1, b * LANES : (b + 1) * LANES]
            mine = jnp.sum(jnp.where(own == ids, rank, 0.0), axis=0, keepdims=True)
            dest_ref[k : k + 1, b * LANES : (b + 1) * LANES] = own * capacity + mine.astype(i32)
    total = jnp.zeros((2 * rows, LANES), f32)
    for k in range(stencil):
        dest = dest_ref[k : k + 1, :]
        node = node_ref[k : k + 1, :]
        place = iota((rows, points), 0) == dest // LANES
        upper = (node // LANES + 1).astype(f32)
        lower = (node % LANES).astype(f32)
        left = jnp.concatenate(
            [jnp.where(place, upper, 0.0), jnp.where(place, lower, 0.0)], axis=0
        ).astype(bf16)
        right = jnp.where(iota((LANES, points), 0) == dest % LANES, 1.0, 0.0).astype(bf16)
        total = total + dot(left, right, NT)
    req_ref[...] = (total[:rows] * LANES + total[rows:]).astype(i32)
    copy(req_ref, req_hbm)
    copies[0].wait()
    copies[1].wait()
    nodes, width = disp_ref.shape[1], disp_ref.shape[2]
    half = width // 2
    for c in range(6):
        field = disp_ref[c] if c < 3 else vel_ref[c - 3]
        turned = field.T
        if c < 3:
            ends = (field[nodes - 1 :, :], field[:1, :])
            span_a[3 * fields, c : c + 1, :] = jnp.where(odd_x == 0, *ends)
            span_b[3 * fields, c : c + 1, :] = jnp.where(odd_x == 1, *ends)
            ends = (turned[width - 1 :, :], turned[:1, :])
            chord_a[2 * cells_x, c : c + 1, :] = jnp.where(odd_y == 0, *ends)
            chord_b[2 * cells_x, c : c + 1, :] = jnp.where(odd_y == 1, *ends)
        for n, part in enumerate(split(turned)):
            for h in range(2):
                first = (6 * n + c) * half
                table_ref[first : first + half, h * nodes : (h + 1) * nodes] = part[
                    h * half : (h + 1) * half
                ]
    for one in copies[2:]:
        one.wait()


def slots_kernel(dest_ref, weight_ref, slots_ref):
    stencil, points = dest_ref.shape
    rows = slots_ref.shape[1]
    total = jnp.zeros((4 * rows, LANES), f32)
    point = iota((1, points), 1)
    point_a = (point // LANES).astype(f32)
    point_b = (point % LANES).astype(f32)
    for k in range(stencil):
        dest = dest_ref[k : k + 1, :]
        high, low = split(weight_ref[k : k + 1, :])
        place = iota((rows, points), 0) == dest // LANES
        parts = [point_a, point_b, high.astype(f32), low.astype(f32)]
        left = jnp.concatenate([jnp.where(place, part, 0.0) for part in parts], axis=0)
        right = jnp.where(iota((LANES, points), 0) == dest % LANES, 1.0, 0.0).astype(bf16)
        total = total + dot(left.astype(bf16), right, NT)
    slots_ref[0] = total[:rows]
    slots_ref[1] = total[rows : 2 * rows]
    slots_ref[2] = total[2 * rows : 3 * rows] + total[3 * rows :]


def pair(ref, first, start=None):
    if start is None:
        return jnp.concatenate([ref[pl.ds(first, 1), :], ref[pl.ds(first + 1, 1), :]], axis=1)
    return jnp.concatenate(
        [ref[start, pl.ds(first, 1), :], ref[start, pl.ds(first + 1, 1), :]], axis=1
    )


def position(chunk_rows, channels, rows, channel, row):
    if chunk_rows:
        return (row // chunk_rows) * (channels * chunk_rows) + channel * chunk_rows + row % chunk_rows
    return channel * rows + row


def fetch_kernel(chunk_rows, group, asked_ref, table_ref, out_ref):
    rows = asked_ref.shape[0]
    half = table_ref.shape[0] // 12
    double = table_ref.shape[1]
    nodes = double // 2

    def step(g, carry):
        for s in range(group):
            t = g * group + s
            asked = pair(asked_ref, 2 * t)
            lower = asked % LANES
            upper = asked // LANES - 1
            second = lower >= half
            at = jnp.where(upper < 0, -1, jnp.where(second, upper + nodes, upper))
            hot = jnp.where(iota((double, 2 * LANES), 0) == at, 1.0, 0.0).astype(bf16)
            picked = dot(table_ref[...], hot, NN)
            picked = picked[: 6 * half] + picked[6 * half :]
            keep = iota((half, 2 * LANES), 0) == jnp.where(second, lower - half, lower)
            for c in range(6):
                found = jnp.sum(
                    jnp.where(keep, picked[c * half : (c + 1) * half], 0.0), axis=0, keepdims=True
                )
                for h in range(2):
                    to = position(chunk_rows, 6, rows, c, 2 * t + h)
                    out_ref[pl.ds(to, 1), :] = found[:, h * LANES : (h + 1) * LANES]
        return carry

    lax.fori_loop(0, rows // (2 * group), step, 0)


def gather_points(chunk_rows, channels, group, got_ref, slots_ref, g, total):
    rows = slots_ref.shape[1]
    blocks = total.shape[0] // (2 * len(channels))
    lefts, hots = [], []
    for s in range(group):
        row = g * group + s
        weight = slots_ref[2, pl.ds(row, 1), :]
        mine = iota((blocks, LANES), 0).astype(f32) == slots_ref[0, pl.ds(row, 1), :]
        hots.append(
            jnp.where(
                iota((LANES, LANES), 0).astype(f32) == slots_ref[1, pl.ds(row, 1), :], 1.0, 0.0
            ).astype(bf16)
        )
        left = []
        for c in channels:
            value = got_ref[pl.ds(position(chunk_rows, 6, rows, c, row), 1), :]
            for part in split(value * weight):
                left.append(jnp.where(mine, part.astype(f32), 0.0))
        lefts.append(jnp.concatenate(left, axis=0).astype(bf16))
    hots = jnp.concatenate(hots, axis=1)
    return total + dot(jnp.concatenate(lefts, axis=1), hots, NT), hots


def meet_kernel(
    chunk_rows, group, factor, got_ref, slots_ref, base_ref, normals_ref, wall_ref, out_ref, hot_ref
):
    rows = slots_ref.shape[1]
    blocks = base_ref.shape[0]

    def gather(g, total):
        total, hot_ref[g] = gather_points(chunk_rows, (5,), group, got_ref, slots_ref, g, total)
        return total

    total = lax.fori_loop(0, rows // group, gather, jnp.zeros((2 * blocks, LANES), f32))
    wall = total[:blocks] + total[blocks:]
    wall_ref[...] = wall
    pressure = base_ref[...] + factor * wall
    left = []
    for c in range(3):
        normal = jnp.concatenate(
            [normals_ref[c : c + 1, a * LANES : (a + 1) * LANES] for a in range(blocks)], axis=0
        )
        left.extend(part.astype(f32) for part in split(normal * pressure))
    left = jnp.concatenate(left, axis=0).astype(bf16)

    def spread(g, carry):
        seen = dot(left, hot_ref[g], NN)
        for s in range(group):
            row = g * group + s
            at = slice(s * LANES, (s + 1) * LANES)
            weight = slots_ref[2, pl.ds(row, 1), :]
            mine = iota((blocks, LANES), 0).astype(f32) == slots_ref[0, pl.ds(row, 1), :]
            for c in range(3):
                both = (
                    seen[2 * c * blocks : (2 * c + 1) * blocks, at]
                    + seen[(2 * c + 1) * blocks : (2 * c + 2) * blocks, at]
                )
                load = weight * jnp.sum(jnp.where(mine, both, 0.0), axis=0, keepdims=True)
                out_ref[pl.ds(position(chunk_rows, 3, rows, c, row), 1), :] = load
        return carry

    lax.fori_loop(0, rows // group, spread, 0)


def force_kernel(chunk_rows, group, got_ref, asked_ref, base_ref, disp_ref, disp_out, vel_out, total_ref):
    rows = asked_ref.shape[0]
    nodes, width = disp_ref.shape[1], disp_ref.shape[2]
    half_nodes = nodes // 2
    total_ref[...] = jnp.zeros_like(total_ref)

    def step(g, carry):
        lefts, hots = [], []
        for s in range(group):
            row = g * group + s
            asked = asked_ref[pl.ds(row, 1), :]
            upper = asked // LANES - 1
            lower = asked % LANES
            second = upper >= half_nodes
            place = iota((half_nodes, LANES), 0) == jnp.where(second, upper - half_nodes, upper)
            hots.append(
                jnp.where(
                    iota((2 * width, LANES), 0) == jnp.where(second, lower + width, lower), 1.0, 0.0
                ).astype(bf16)
            )
            left = []
            for c in range(3):
                value = got_ref[pl.ds(position(chunk_rows, 3, rows, c, row), 1), :]
                for part in split(value):
                    left.append(jnp.where(place, part.astype(f32), 0.0))
            lefts.append(jnp.concatenate(left, axis=0).astype(bf16))
        total_ref[...] += dot(jnp.concatenate(lefts, axis=1), jnp.concatenate(hots, axis=1), NT)
        return carry

    lax.fori_loop(0, rows // group, step, 0)
    for c in range(3):
        for h in range(2):
            first = total_ref[2 * c * half_nodes : (2 * c + 1) * half_nodes, h * width : (h + 1) * width]
            second = total_ref[(2 * c + 1) * half_nodes : (2 * c + 2) * half_nodes, h * width : (h + 1) * width]
            at = slice(h * half_nodes, (h + 1) * half_nodes)
            vel_next = base_ref[c, at, :] + shell_step * (first + second)
            vel_out[c, at, :] = vel_next
            disp_out[c, at, :] = disp_ref[c, at, :] + shell_step * vel_next


def coef(distance):
    size = jnp.abs(distance)
    value = jnp.where(size == 1, 45.0, jnp.where(size == 2, -9.0, jnp.where(size == 3, 1.0, 0.0)))
    return jnp.where(distance < 0, -value, value)


def flow_kernel(
    disp_ref, vel_ref, fluid_ref, got_xa, got_xb, got_ya, got_yb,
    next_ref, pressure_ref, surface_ref, shell_ref, wide, across, normal, held, sems,
):
    fields, cells_x, cells_y, length = fluid_ref.shape
    nodes, width = disp_ref.shape[1], disp_ref.shape[2]
    copies = []

    def copy(source, target):
        one = pltpu.make_async_copy(source, target, sems.at[len(copies)])
        one.start()
        copies.append(one)

    for c in range(fields):
        copy(fluid_ref.at[c], wide.at[c, pl.ds(3, cells_x)])
    odd_x = lax.axis_index("span") % 2
    odd_y = lax.axis_index("chord") % 2
    for got, side in ((got_xa, 1 - odd_x), (got_xb, odd_x)):
        for c in range(fields):
            wide[c, pl.ds(side * (cells_x + 3), 3)] = got[3 * c : 3 * c + 3]
    ends_x = (got_xa[3 * fields, :8, :], got_xb[3 * fields, :8, :])
    before_x, after_x = jnp.where(odd_x == 1, *ends_x), jnp.where(odd_x == 0, *ends_x)
    ends_y = (got_ya[2 * cells_x], got_yb[2 * cells_x])
    before_y, after_y = jnp.where(odd_y == 1, *ends_y), jnp.where(odd_y == 0, *ends_y)
    row = iota((nodes, width), 0)
    lane = iota((nodes, width), 1)
    for c in range(3):
        field = disp_ref[c]

        def column(plane, at):
            only = jnp.where(iota((8, width), 0) == c, plane, 0.0)
            place = jnp.where(iota((8, width), 1) == at, 1.0, 0.0).astype(bf16)
            high, low = split(only)
            return dot(high, place, TN) + dot(low, place, TN)

        left = column(before_y, 0)
        right = column(after_y, width - 1)
        above = jnp.where(row == 0, before_x[c : c + 1, :], pltpu.roll(field, 1, 0))
        below = jnp.where(
            row == nodes - 1, after_x[c : c + 1, :], pltpu.roll(field, nodes - 1, 0)
        )
        west = jnp.where(lane == 0, left, pltpu.roll(field, 1, 1))
        east = jnp.where(lane == width - 1, right, pltpu.roll(field, width - 1, 1))
        bending = above + below + west + east - 4.0 * field
        vel = vel_ref[c]
        shell_ref[c] = vel + shell_step * (stiffness * bending - damping * vel)
    source = iota((length, length), 0)
    target = iota((length, length), 1)
    inner = coef(source - target)
    ghost = jnp.where(source < 3, coef(-(source + 1 + target)), 0.0)
    for one in copies:
        one.wait()
    flat = cells_x * cells_y
    for n, field, table in ((0, 0, inner + ghost), (1, 3, inner - ghost)):
        table = table.astype(bf16)
        high, low = split(wide[field, 3 : 3 + cells_x].reshape(flat, length))
        total = dot(jnp.concatenate([high, low], axis=1), jnp.concatenate([table, table], axis=0), NN)
        normal[n] = (total * (1.0 / 60.0)).reshape(cells_x, cells_y, length)

    per = LANES // cells_y
    target = iota((LANES, LANES), 0)
    source = iota((LANES, LANES), 1)
    same = jnp.where(target // cells_y == source // cells_y, coef(source - target), 0.0)
    target = iota((LANES, 8 * per), 0)
    source = iota((LANES, 8 * per), 1)
    near_plane = target // cells_y == source // 8
    below_y = jnp.where(near_plane, coef(source % 8 - 8 - target % cells_y), 0.0)
    above_y = jnp.where(near_plane, coef(cells_y + source % 8 - target % cells_y), 0.0)
    chord_table = jnp.concatenate([same, same, below_y, below_y, above_y, above_y], axis=1).astype(bf16)
    for n, field in enumerate((0, 2)):
        for g in range(cells_x // per):
            inner_rows = wide[field, 3 + g * per : 3 + (g + 1) * per].reshape(LANES, length)
            at = slice(n * cells_x + g * per, n * cells_x + (g + 1) * per)
            ends = (got_ya[at].reshape(8 * per, length), got_yb[at].reshape(8 * per, length))
            parts = split(inner_rows) + split(jnp.where(odd_y == 1, *ends)) + split(jnp.where(odd_y == 0, *ends))
            total = dot(chord_table, jnp.concatenate(parts, axis=0), NN) * (1.0 / 60.0)
            across[n, g * per : (g + 1) * per] = total.reshape(per, cells_y, length)

    def central(window):
        return (
            0.75 * (window(1) - window(-1)) - 0.15 * (window(2) - window(-2))
        ) + (1.0 / 60.0) * (window(3) - window(-3))

    def plane(x):
        def along_x(field):
            return central(lambda offset: wide[field, x + 3 + offset])

        x_p = along_x(0)
        x_u = along_x(1)
        pressure_ref[x] = wide[0, x + 3] + time_step * (
            -flow_speed * x_p - (x_u + across[1, x] + normal[1, x])
        )
        held[0, x] = wide[1, x + 3] + time_step * (-flow_speed * x_u - x_p)
        held[1, x] = wide[2, x + 3] + time_step * (-flow_speed * along_x(2) - across[0, x])
        held[2, x] = wide[3, x + 3] + time_step * (-flow_speed * along_x(3) - normal[0, x])

    parts = 4
    size = cells_x // parts
    copies = []
    for part in range(parts):

        def planes(i, carry):
            plane(part * size + 2 * i)
            plane(part * size + 2 * i + 1)
            return carry

        lax.fori_loop(0, size // 2, planes, 0)
        at = pl.ds(part * size, size)
        one = pltpu.make_async_copy(held.at[:, at], next_ref.at[pl.ds(1, 3), at], sems.at[part])
        one.start()
        copies.append(one)
    lead = jnp.where((iota((8, length), 0) == 0) & (iota((8, length), 1) == 0), 1.0, 0.0).astype(bf16)
    blocks = surface_ref.shape[0]
    for b in range(blocks):
        high, low = split(pressure_ref[b * per : (b + 1) * per].reshape(LANES, length))
        found = dot(lead, high, NT) + dot(lead, low, NT)
        surface_ref[b : b + 1, :] = found[:1]
    for one in copies:
        one.wait()


def wall_kernel(
    chunk_rows, group, got_ref, slots_ref, wall_ref, pressure_ref, next_in, next_out, motion_ref
):
    blocks = wall_ref.shape[0]
    channels = (0, 1, 2, 3, 4)

    def gather(g, total):
        return gather_points(chunk_rows, channels, group, got_ref, slots_ref, g, total)[0]

    groups = slots_ref.shape[1] // group
    total = lax.fori_loop(0, groups, gather, jnp.zeros((10 * blocks, LANES), f32))
    for c in range(6):
        if c < 5:
            value = total[2 * c * blocks : (2 * c + 1) * blocks] + total[(2 * c + 1) * blocks : (2 * c + 2) * blocks]
        else:
            value = wall_ref[...]
        for a in range(blocks):
            motion_ref[c : c + 1, a * LANES : (a + 1) * LANES] = value[a : a + 1]
    del next_in
    _, cells_x, cells_y, length = next_out.shape
    target = iota((8, length), 1)
    row = jnp.zeros((8, length), f32)
    for j in range(3):
        row = row + coef(-(j + 1 + target))
    row = jnp.where(iota((8, length), 0) == 0, row, 0.0).astype(bf16)
    per = LANES // cells_y
    for b in range(cells_x // per):
        wall = jnp.where(
            iota((8, LANES), 0) == 0, wall_ref[b : b + 1, :] * (-2.0 * time_step / 60.0), 0.0
        )
        high, low = split(wall)
        added = dot(high, row, TN) + dot(low, row, TN)
        at = slice(b * per, (b + 1) * per)
        next_out[0, at] = pressure_ref[at] + added.reshape(per, cells_y, length)


def exchange(value, devices, channels, chunk_rows, rows, capacity):
    if chunk_rows:
        shape = (devices, 1, channels * chunk_rows * LANES)
        got = lax.all_to_all(value.reshape(shape), AXES, split_axis=0, concat_axis=0, tiled=True)
        return got.reshape(channels * rows, LANES)
    value = value.reshape(channels, devices, capacity).transpose(1, 0, 2)
    got = lax.all_to_all(value, AXES, split_axis=0, concat_axis=0, tiled=True)
    return got.transpose(1, 0, 2).reshape(channels * rows, LANES)


def body(fluid_state, shell_disp, shell_vel, owners, node_local, rbf_weight, normals):
    span_count = lax.axis_size("span")
    chord_count = lax.axis_size("chord")
    devices = span_count * chord_count
    points, stencil = owners.shape
    capacity = max(2, (2 * points * stencil + devices - 1) // devices)
    rows = devices * capacity // LANES
    chunk_rows = capacity // LANES if capacity % LANES == 0 else 0
    blocks = points // LANES
    fields, cells_x, cells_y, length = fluid_state.shape
    _, nodes, width = shell_disp.shape
    sds = jax.ShapeDtypeStruct
    vmem = pl.BlockSpec(memory_space=pltpu.VMEM)
    hbm = pl.BlockSpec(memory_space=pl.ANY)

    near_out = pltpu.VMEM
    span_shape = near_out((3 * fields + 1, cells_y, length), f32)
    chord_shape = near_out((2 * cells_x + 1, 8, length), f32)
    requests, dest, table, span_a, span_b, chord_a, chord_b = call(
        functools.partial(route_kernel, devices, capacity),
        [
            sds((rows, LANES), i32),
            near_out((stencil, points), i32),
            near_out((6 * width, 2 * nodes), bf16),
            span_shape,
            span_shape,
            chord_shape,
            chord_shape,
        ],
        owners.T,
        node_local.T,
        shell_disp,
        shell_vel,
        fluid_state,
        flops=100_000_000,
        in_specs=[vmem, vmem, hbm, hbm, hbm],
        out_specs=[hbm] + [vmem] * 6,
        scratch_shapes=[
            pltpu.VMEM((rows, LANES), i32),
            pltpu.VMEM(shell_disp.shape, f32),
            pltpu.VMEM(shell_vel.shape, f32),
            pltpu.SemaphoreType.DMA((2 * fields + 7,)),
        ],
    )

    def swapped(one, two, axis, size):
        even = [pair for i in range(0, size - 1, 2) for pair in ((i, i + 1), (i + 1, i))]
        odd = [pair for i in range(1, size - 1, 2) for pair in ((i, i + 1), (i + 1, i))]
        first = lax.ppermute(one, axis, even)
        return first, lax.ppermute(two, axis, odd)

    got_xa, got_xb = swapped(span_a, span_b, "span", span_count)
    got_ya, got_yb = swapped(chord_a, chord_b, "chord", chord_count)

    asked = exchange(requests, devices, 1, chunk_rows, rows, capacity)

    slots = call(
        slots_kernel,
        near_out((3, rows, LANES), f32),
        dest,
        rbf_weight.T,
        held=(0,),
        flops=200_000_000,
    )
    flow_next, pressure, surface, shell_base = call(
        flow_kernel,
        [
            sds(fluid_state.shape, f32),
            near_out((cells_x, cells_y, length), f32),
            near_out((blocks, LANES), f32),
            near_out(shell_disp.shape, f32),
        ],
        shell_disp,
        shell_vel,
        fluid_state,
        got_xa,
        got_xb,
        got_ya,
        got_yb,
        flops=300_000_000,
        held=(0, 1, 3, 4, 5, 6),
        in_specs=[vmem, vmem, hbm, vmem, vmem, vmem, vmem],
        out_specs=[hbm, vmem, vmem, vmem],
        scratch_shapes=[
            pltpu.VMEM((fields, cells_x + 6, cells_y, length), f32),
            pltpu.VMEM((2, cells_x, cells_y, length), f32),
            pltpu.VMEM((2, cells_x, cells_y, length), f32),
            pltpu.VMEM((3, cells_x, cells_y, length), f32),
            pltpu.SemaphoreType.DMA((fields + 2,)),
        ],
    )

    picked = call(
        functools.partial(fetch_kernel, chunk_rows, 32),
        near_out((6 * rows, LANES), f32),
        asked,
        table,
        held=(0, 1),
        flops=3_000_000_000,
    )
    replies = exchange(picked, devices, 6, chunk_rows, rows, capacity)

    wall_first = 2.0 * (-45.0 + 9.0 - 1.0) / 60.0
    group = 32
    wall, loads = call(
        functools.partial(meet_kernel, chunk_rows, group, -time_step * wall_first),
        [
            near_out((blocks, LANES), f32),
            sds((3 * rows, LANES), f32),
        ],
        replies,
        slots,
        surface,
        normals,
        held=(0, 1, 2, 3),
        flops=300_000_000,
        scratch_shapes=[pltpu.VMEM((rows // group, LANES, group * LANES), bf16)],
    )
    arrived = exchange(loads, devices, 3, chunk_rows, rows, capacity)

    block = pl.BlockSpec((1, cells_x, cells_y, length), lambda i: (0, 0, 0, 0))
    fluid_next, interface_motion = call(
        functools.partial(wall_kernel, chunk_rows, group),
        [sds(fluid_state.shape, f32), sds((6, points), f32)],
        replies,
        slots,
        wall,
        pressure,
        flow_next,
        flops=200_000_000,
        held=(0, 1, 2, 3),
        grid=(1,),
        in_specs=[vmem, vmem, vmem, vmem, hbm],
        out_specs=[block, vmem],
        input_output_aliases={4: 0},
    )

    disp_next, vel_next = call(
        functools.partial(force_kernel, chunk_rows, 64),
        [sds(shell_disp.shape, f32), sds(shell_vel.shape, f32)],
        arrived,
        asked,
        shell_base,
        shell_disp,
        held=(0, 1, 2, 3),
        flops=3_000_000_000,
        scratch_shapes=[pltpu.VMEM((3 * nodes, 2 * width), f32)],
    )
    return (fluid_next, interface_motion, disp_next, vel_next)


def solution(mesh):
    placed = (
        P(None, "span", "chord", None),
        P(None, "span", "chord"),
        P(None, "span", "chord"),
        P(AXES, None),
        P(AXES, None),
        P(AXES, None),
        P(None, AXES),
    )

    return jax.shard_map(
        body,
        mesh=mesh,
        in_specs=placed,
        out_specs=(
            P(None, "span", "chord", None),
            P(None, AXES),
            P(None, "span", "chord"),
            P(None, "span", "chord"),
        ),
        check_vma=False,
    )
```

```python
import functools

import jax
import jax.numpy as jnp
from jax import lax
from jax.experimental import pallas as pl
from jax.experimental.pallas import tpu as pltpu
from jax.sharding import PartitionSpec as P


flow_speed = 0.5
time_step = 0.4
stiffness = 0.5
damping = 0.2
shell_step = 0.3

AXES = ("span", "chord")
LANES = 128
f32 = jnp.float32
bf16 = jnp.bfloat16
i32 = jnp.int32
NT = (((1,), (1,)), ((), ()))
TN = (((0,), (0,)), ((), ()))
NN = (((1,), (0,)), ((), ()))


def dot(a, b, dims, precision=None):
    return lax.dot_general(a, b, dims, precision=precision, preferred_element_type=f32)


def iota(shape, dim):
    return lax.broadcasted_iota(i32, shape, dim)


def split(value):
    high = value.astype(bf16)
    low = (value - high.astype(f32)).astype(bf16)
    return high, low


def near(value):
    return pltpu.with_memory_space_constraint(value, pltpu.VMEM)


def call(kernel, outs, *args, flops=1_000_000, held=(), **kw):
    single = not isinstance(outs, (list, tuple))
    space = pl.BlockSpec(memory_space=pltpu.VMEM)
    kw.setdefault("in_specs", [space] * len(args))
    args = [near(a) if n in held else a for n, a in enumerate(args)]
    kw.setdefault("out_specs", space if single else [space] * len(outs))
    nbytes = sum(a.size * a.dtype.itemsize for a in args)
    return pl.pallas_call(
        kernel,
        out_shape=outs,
        cost_estimate=pl.CostEstimate(flops=flops, transcendentals=0, bytes_accessed=nbytes),
        **kw,
    )(*args)


def route_kernel(
    devices, capacity, own_ref, node_ref, disp_hbm, vel_hbm, fluid_ref,
    req_hbm, dest_ref, table_ref, span_a, span_b, chord_a, chord_b,
    req_ref, disp_ref, vel_ref, sems,
):
    fields, cells_x, cells_y, _ = fluid_ref.shape
    copies = []

    def copy(source, target):
        one = pltpu.make_async_copy(source, target, sems.at[len(copies)])
        one.start()
        copies.append(one)

    copy(disp_hbm, disp_ref)
    copy(vel_hbm, vel_ref)
    odd_x = lax.axis_index("span") % 2
    odd_y = lax.axis_index("chord") % 2
    for c in range(fields):
        copy(fluid_ref.at[c, pl.ds((1 - odd_x) * (cells_x - 3), 3)], span_a.at[pl.ds(3 * c, 3)])
        copy(fluid_ref.at[c, pl.ds(odd_x * (cells_x - 3), 3)], span_b.at[pl.ds(3 * c, 3)])
    for n, c in enumerate((0, 2)):
        first = pl.multiple_of((1 - odd_y) * (cells_y - 8), 8)
        copy(fluid_ref.at[c, :, pl.ds(first, 8)], chord_a.at[pl.ds(n * cells_x, cells_x)])
        first = pl.multiple_of(odd_y * (cells_y - 8), 8)
        copy(fluid_ref.at[c, :, pl.ds(first, 8)], chord_b.at[pl.ds(n * cells_x, cells_x)])
    stencil, points = own_ref.shape
    blocks = points // LANES
    rows = req_ref.shape[0]
    member = []
    for b in range(blocks):
        ids = iota((devices, LANES), 0)
        hit = jnp.zeros((devices, LANES), f32)
        for k in range(stencil):
            hit = jnp.where(own_ref[k : k + 1, b * LANES : (b + 1) * LANES] == ids, 1.0, hit)
        member.append(hit)
    stacked = jnp.concatenate(member, axis=0).astype(bf16)
    source = iota((LANES, 2 * LANES), 0)
    target = iota((LANES, 2 * LANES), 1)
    table = jnp.where((source < target) | (target >= LANES), 1.0, 0.0).astype(bf16)
    counted = dot(stacked, table, NN)
    offset = jnp.zeros((devices, LANES), f32)
    for b in range(blocks):
        part = counted[b * devices : (b + 1) * devices]
        rank = part[:, :LANES] + offset
        offset = offset + part[:, LANES:]
        ids = iota((devices, LANES), 0)
        for k in range(stencil):
            own = own_ref[k : k + 1, b * LANES : (b + 1) * LANES]
            mine = jnp.sum(jnp.where(own == ids, rank, 0.0), axis=0, keepdims=True)
            dest_ref[k : k + 1, b * LANES : (b + 1) * LANES] = own * capacity + mine.astype(i32)
    total = jnp.zeros((2 * rows, LANES), f32)
    for k in range(stencil):
        dest = dest_ref[k : k + 1, :]
        node = node_ref[k : k + 1, :]
        place = iota((rows, points), 0) == dest // LANES
        upper = (node // LANES + 1).astype(f32)
        lower = (node % LANES).astype(f32)
        left = jnp.concatenate(
            [jnp.where(place, upper, 0.0), jnp.where(place, lower, 0.0)], axis=0
        ).astype(bf16)
        right = jnp.where(iota((LANES, points), 0) == dest % LANES, 1.0, 0.0).astype(bf16)
        total = total + dot(left, right, NT)
    req_ref[...] = (total[:rows] * LANES + total[rows:]).astype(i32)
    copy(req_ref, req_hbm)
    copies[0].wait()
    copies[1].wait()
    nodes, width = disp_ref.shape[1], disp_ref.shape[2]
    half = width // 2
    channels = table_ref.shape[0] // (2 * half)
    for c in range(6):
        field = disp_ref[c] if c < 3 else vel_ref[c - 3]
        turned = field.T
        if c < 3:
            ends = (field[nodes - 1 :, :], field[:1, :])
            span_a[3 * fields, c : c + 1, :] = jnp.where(odd_x == 0, *ends)
            span_b[3 * fields, c : c + 1, :] = jnp.where(odd_x == 1, *ends)
            ends = (turned[width - 1 :, :], turned[:1, :])
            chord_a[2 * cells_x, c : c + 1, :] = jnp.where(odd_y == 0, *ends)
            chord_b[2 * cells_x, c : c + 1, :] = jnp.where(odd_y == 1, *ends)
        for n, part in enumerate(split(turned)):
            for h in range(2 if c >= 6 - channels else 0):
                first = (channels * n + c - 6 + channels) * half
                table_ref[first : first + half, h * nodes : (h + 1) * nodes] = part[
                    h * half : (h + 1) * half
                ]
    for one in copies[2:]:
        one.wait()


def slots_kernel(dest_ref, weight_ref, slots_ref):
    stencil, points = dest_ref.shape
    rows = slots_ref.shape[1]
    total = jnp.zeros((4 * rows, LANES), f32)
    point = iota((1, points), 1)
    point_a = (point // LANES).astype(f32)
    point_b = (point % LANES).astype(f32)
    for k in range(stencil):
        dest = dest_ref[k : k + 1, :]
        high, low = split(weight_ref[k : k + 1, :])
        place = iota((rows, points), 0) == dest // LANES
        parts = [point_a, point_b, high.astype(f32), low.astype(f32)]
        left = jnp.concatenate([jnp.where(place, part, 0.0) for part in parts], axis=0)
        right = jnp.where(iota((LANES, points), 0) == dest % LANES, 1.0, 0.0).astype(bf16)
        total = total + dot(left.astype(bf16), right, NT)
    slots_ref[0] = total[:rows]
    slots_ref[1] = total[rows : 2 * rows]
    slots_ref[2] = total[2 * rows : 3 * rows] + total[3 * rows :]


def pair(ref, first, start=None):
    if start is None:
        return jnp.concatenate([ref[pl.ds(first, 1), :], ref[pl.ds(first + 1, 1), :]], axis=1)
    return jnp.concatenate(
        [ref[start, pl.ds(first, 1), :], ref[start, pl.ds(first + 1, 1), :]], axis=1
    )


def position(chunk_rows, channels, rows, channel, row):
    if chunk_rows:
        return (row // chunk_rows) * (channels * chunk_rows) + channel * chunk_rows + row % chunk_rows
    return channel * rows + row


def fetch_kernel(chunk_rows, group, asked_ref, table_ref, disp_ref, out_ref):
    rows = asked_ref.shape[0]
    nodes, width = disp_ref.shape[1], disp_ref.shape[2]
    half = width // 2
    channels = table_ref.shape[0] // (2 * half)
    straight = 6 - channels

    def step(g, carry):
        for s in range(group):
            t = g * group + s
            asked = pair(asked_ref, 2 * t)
            lower = asked % LANES
            upper = asked // LANES - 1
            second = lower >= half
            at = jnp.where(upper < 0, -1, jnp.where(second, upper + nodes, upper))
            hot = jnp.where(iota((2 * nodes, 2 * LANES), 0) == at, 1.0, 0.0).astype(bf16)
            picked = dot(table_ref[...], hot, NN)
            picked = picked[: channels * half] + picked[channels * half :]
            keep = iota((half, 2 * LANES), 0) == jnp.where(second, lower - half, lower)
            for c in range(channels):
                found = jnp.sum(
                    jnp.where(keep, picked[c * half : (c + 1) * half], 0.0), axis=0, keepdims=True
                )
                for h in range(2):
                    to = position(chunk_rows, 6, rows, straight + c, 2 * t + h)
                    out_ref[pl.ds(to, 1), :] = found[:, h * LANES : (h + 1) * LANES]
            for h in range(2):
                one = asked_ref[pl.ds(2 * t + h, 1), :]
                lane = jnp.broadcast_to(one % LANES, (8, LANES))
                line = one // LANES - 1
                for c in range(straight):
                    total = jnp.zeros((8, LANES), f32)
                    for block in range(nodes // 8):
                        seen = jnp.take_along_axis(
                            disp_ref[c, block * 8 : (block + 1) * 8, :], lane, axis=1,
                            mode="promise_in_bounds",
                        )
                        here = iota((8, LANES), 0) + block * 8 == line
                        total = jnp.where(here, seen, total)
                    to = position(chunk_rows, 6, rows, c, 2 * t + h)
                    out_ref[pl.ds(to, 1), :] = jnp.sum(total, axis=0, keepdims=True)
        return carry

    lax.fori_loop(0, rows // (2 * group), step, 0)


def gather_points(chunk_rows, channels, group, got_ref, slots_ref, g, total):
    rows = slots_ref.shape[1]
    blocks = total.shape[0] // (2 * len(channels))
    lefts, hots = [], []
    for s in range(group):
        row = g * group + s
        weight = slots_ref[2, pl.ds(row, 1), :]
        mine = iota((blocks, LANES), 0).astype(f32) == slots_ref[0, pl.ds(row, 1), :]
        hots.append(
            jnp.where(
                iota((LANES, LANES), 0).astype(f32) == slots_ref[1, pl.ds(row, 1), :], 1.0, 0.0
            ).astype(bf16)
        )
        left = []
        for c in channels:
            value = got_ref[pl.ds(position(chunk_rows, 6, rows, c, row), 1), :]
            for part in split(value * weight):
                left.append(jnp.where(mine, part.astype(f32), 0.0))
        lefts.append(jnp.concatenate(left, axis=0).astype(bf16))
    hots = jnp.concatenate(hots, axis=1)
    return total + dot(jnp.concatenate(lefts, axis=1), hots, NT), hots


def meet_kernel(
    chunk_rows, group, factor, got_ref, slots_ref, base_ref, normals_ref, wall_ref, out_ref, hot_ref
):
    rows = slots_ref.shape[1]
    blocks = base_ref.shape[0]

    def gather(g, total):
        total, hot_ref[g] = gather_points(chunk_rows, (5,), group, got_ref, slots_ref, g, total)
        return total

    total = lax.fori_loop(0, rows // group, gather, jnp.zeros((2 * blocks, LANES), f32))
    wall = total[:blocks] + total[blocks:]
    wall_ref[...] = wall
    pressure = base_ref[...] + factor * wall
    left = []
    for c in range(3):
        normal = jnp.concatenate(
            [normals_ref[c : c + 1, a * LANES : (a + 1) * LANES] for a in range(blocks)], axis=0
        )
        left.extend(part.astype(f32) for part in split(normal * pressure))
    left = jnp.concatenate(left, axis=0).astype(bf16)

    def spread(g, carry):
        seen = dot(left, hot_ref[g], NN)
        for s in range(group):
            row = g * group + s
            at = slice(s * LANES, (s + 1) * LANES)
            weight = slots_ref[2, pl.ds(row, 1), :]
            mine = iota((blocks, LANES), 0).astype(f32) == slots_ref[0, pl.ds(row, 1), :]
            for c in range(3):
                both = (
                    seen[2 * c * blocks : (2 * c + 1) * blocks, at]
                    + seen[(2 * c + 1) * blocks : (2 * c + 2) * blocks, at]
                )
                load = weight * jnp.sum(jnp.where(mine, both, 0.0), axis=0, keepdims=True)
                out_ref[pl.ds(position(chunk_rows, 3, rows, c, row), 1), :] = load
        return carry

    lax.fori_loop(0, rows // group, spread, 0)


def force_kernel(chunk_rows, group, got_ref, asked_ref, base_ref, disp_ref, disp_out, vel_out, total_ref):
    rows = asked_ref.shape[0]
    nodes, width = disp_ref.shape[1], disp_ref.shape[2]
    half_nodes = nodes // 2
    total_ref[...] = jnp.zeros_like(total_ref)

    def step(g, carry):
        lefts, hots = [], []
        for s in range(group):
            row = g * group + s
            asked = asked_ref[pl.ds(row, 1), :]
            upper = asked // LANES - 1
            lower = asked % LANES
            second = upper >= half_nodes
            place = iota((half_nodes, LANES), 0) == jnp.where(second, upper - half_nodes, upper)
            hots.append(
                jnp.where(
                    iota((2 * width, LANES), 0) == jnp.where(second, lower + width, lower), 1.0, 0.0
                ).astype(bf16)
            )
            left = []
            for c in range(3):
                value = got_ref[pl.ds(position(chunk_rows, 3, rows, c, row), 1), :]
                for part in split(value):
                    left.append(jnp.where(place, part.astype(f32), 0.0))
            lefts.append(jnp.concatenate(left, axis=0).astype(bf16))
        total_ref[...] += dot(jnp.concatenate(lefts, axis=1), jnp.concatenate(hots, axis=1), NT)
        return carry

    lax.fori_loop(0, rows // group, step, 0)
    for c in range(3):
        for h in range(2):
            first = total_ref[2 * c * half_nodes : (2 * c + 1) * half_nodes, h * width : (h + 1) * width]
            second = total_ref[(2 * c + 1) * half_nodes : (2 * c + 2) * half_nodes, h * width : (h + 1) * width]
            at = slice(h * half_nodes, (h + 1) * half_nodes)
            vel_next = base_ref[c, at, :] + shell_step * (first + second)
            vel_out[c, at, :] = vel_next
            disp_out[c, at, :] = disp_ref[c, at, :] + shell_step * vel_next


def coef(distance):
    size = jnp.abs(distance)
    value = jnp.where(size == 1, 45.0, jnp.where(size == 2, -9.0, jnp.where(size == 3, 1.0, 0.0)))
    return jnp.where(distance < 0, -value, value)


def flow_kernel(
    disp_ref, vel_ref, fluid_ref, got_xa, got_xb, got_ya, got_yb,
    next_ref, pressure_ref, surface_ref, shell_ref, wide, across, normal, held, sems,
):
    fields, cells_x, cells_y, length = fluid_ref.shape
    nodes, width = disp_ref.shape[1], disp_ref.shape[2]
    copies = []

    def copy(source, target):
        one = pltpu.make_async_copy(source, target, sems.at[len(copies)])
        one.start()
        copies.append(one)

    for c in range(fields):
        copy(fluid_ref.at[c], wide.at[c, pl.ds(3, cells_x)])
    odd_x = lax.axis_index("span") % 2
    odd_y = lax.axis_index("chord") % 2
    for got, side in ((got_xa, 1 - odd_x), (got_xb, odd_x)):
        for c in range(fields):
            wide[c, pl.ds(side * (cells_x + 3), 3)] = got[3 * c : 3 * c + 3]
    ends_x = (got_xa[3 * fields, :8, :], got_xb[3 * fields, :8, :])
    before_x, after_x = jnp.where(odd_x == 1, *ends_x), jnp.where(odd_x == 0, *ends_x)
    ends_y = (got_ya[2 * cells_x], got_yb[2 * cells_x])
    before_y, after_y = jnp.where(odd_y == 1, *ends_y), jnp.where(odd_y == 0, *ends_y)
    row = iota((nodes, width), 0)
    lane = iota((nodes, width), 1)
    for c in range(3):
        field = disp_ref[c]

        def column(plane, at):
            only = jnp.where(iota((8, width), 0) == c, plane, 0.0)
            place = jnp.where(iota((8, width), 1) == at, 1.0, 0.0).astype(bf16)
            high, low = split(only)
            return dot(high, place, TN) + dot(low, place, TN)

        left = column(before_y, 0)
        right = column(after_y, width - 1)
        above = jnp.where(row == 0, before_x[c : c + 1, :], pltpu.roll(field, 1, 0))
        below = jnp.where(
            row == nodes - 1, after_x[c : c + 1, :], pltpu.roll(field, nodes - 1, 0)
        )
        west = jnp.where(lane == 0, left, pltpu.roll(field, 1, 1))
        east = jnp.where(lane == width - 1, right, pltpu.roll(field, width - 1, 1))
        bending = above + below + west + east - 4.0 * field
        vel = vel_ref[c]
        shell_ref[c] = vel + shell_step * (stiffness * bending - damping * vel)
    source = iota((length, length), 0)
    target = iota((length, length), 1)
    inner = coef(source - target)
    ghost = jnp.where(source < 3, coef(-(source + 1 + target)), 0.0)
    for one in copies:
        one.wait()
    flat = cells_x * cells_y
    for n, field, table in ((0, 0, inner + ghost), (1, 3, inner - ghost)):
        table = table.astype(bf16)
        high, low = split(wide[field, 3 : 3 + cells_x].reshape(flat, length))
        total = dot(jnp.concatenate([high, low], axis=1), jnp.concatenate([table, table], axis=0), NN)
        normal[n] = (total * (1.0 / 60.0)).reshape(cells_x, cells_y, length)

    per = LANES // cells_y
    target = iota((LANES, LANES), 0)
    source = iota((LANES, LANES), 1)
    same = jnp.where(target // cells_y == source // cells_y, coef(source - target), 0.0)
    target = iota((LANES, 8 * per), 0)
    source = iota((LANES, 8 * per), 1)
    near_plane = target // cells_y == source // 8
    below_y = jnp.where(near_plane, coef(source % 8 - 8 - target % cells_y), 0.0)
    above_y = jnp.where(near_plane, coef(cells_y + source % 8 - target % cells_y), 0.0)
    chord_table = jnp.concatenate([same, same, below_y, below_y, above_y, above_y], axis=1).astype(bf16)
    for n, field in enumerate((0, 2)):
        for g in range(cells_x // per):
            inner_rows = wide[field, 3 + g * per : 3 + (g + 1) * per].reshape(LANES, length)
            at = slice(n * cells_x + g * per, n * cells_x + (g + 1) * per)
            ends = (got_ya[at].reshape(8 * per, length), got_yb[at].reshape(8 * per, length))
            parts = split(inner_rows) + split(jnp.where(odd_y == 1, *ends)) + split(jnp.where(odd_y == 0, *ends))
            total = dot(chord_table, jnp.concatenate(parts, axis=0), NN) * (1.0 / 60.0)
            across[n, g * per : (g + 1) * per] = total.reshape(per, cells_y, length)

    def central(window):
        return (
            0.75 * (window(1) - window(-1)) - 0.15 * (window(2) - window(-2))
        ) + (1.0 / 60.0) * (window(3) - window(-3))

    def plane(x):
        def along_x(field):
            return central(lambda offset: wide[field, x + 3 + offset])

        x_p = along_x(0)
        x_u = along_x(1)
        pressure_ref[x] = wide[0, x + 3] + time_step * (
            -flow_speed * x_p - (x_u + across[1, x] + normal[1, x])
        )
        held[0, x] = wide[1, x + 3] + time_step * (-flow_speed * x_u - x_p)
        held[1, x] = wide[2, x + 3] + time_step * (-flow_speed * along_x(2) - across[0, x])
        held[2, x] = wide[3, x + 3] + time_step * (-flow_speed * along_x(3) - normal[0, x])

    parts = 4
    size = cells_x // parts
    copies = []
    for part in range(parts):

        def planes(i, carry):
            plane(part * size + 2 * i)
            plane(part * size + 2 * i + 1)
            return carry

        lax.fori_loop(0, size // 2, planes, 0)
        at = pl.ds(part * size, size)
        one = pltpu.make_async_copy(held.at[:, at], next_ref.at[pl.ds(1, 3), at], sems.at[part])
        one.start()
        copies.append(one)
    lead = jnp.where((iota((8, length), 0) == 0) & (iota((8, length), 1) == 0), 1.0, 0.0).astype(bf16)
    blocks = surface_ref.shape[0]
    for b in range(blocks):
        high, low = split(pressure_ref[b * per : (b + 1) * per].reshape(LANES, length))
        found = dot(lead, high, NT) + dot(lead, low, NT)
        surface_ref[b : b + 1, :] = found[:1]
    for one in copies:
        one.wait()


def wall_kernel(
    chunk_rows, group, got_ref, slots_ref, wall_ref, pressure_ref, next_in, next_out, motion_ref
):
    blocks = wall_ref.shape[0]
    channels = (0, 1, 2, 3, 4)

    def gather(g, total):
        return gather_points(chunk_rows, channels, group, got_ref, slots_ref, g, total)[0]

    groups = slots_ref.shape[1] // group
    total = lax.fori_loop(0, groups, gather, jnp.zeros((10 * blocks, LANES), f32))
    for c in range(6):
        if c < 5:
            value = total[2 * c * blocks : (2 * c + 1) * blocks] + total[(2 * c + 1) * blocks : (2 * c + 2) * blocks]
        else:
            value = wall_ref[...]
        for a in range(blocks):
            motion_ref[c : c + 1, a * LANES : (a + 1) * LANES] = value[a : a + 1]
    del next_in
    _, cells_x, cells_y, length = next_out.shape
    target = iota((8, length), 1)
    row = jnp.zeros((8, length), f32)
    for j in range(3):
        row = row + coef(-(j + 1 + target))
    row = jnp.where(iota((8, length), 0) == 0, row, 0.0).astype(bf16)
    per = LANES // cells_y
    for b in range(cells_x // per):
        wall = jnp.where(
            iota((8, LANES), 0) == 0, wall_ref[b : b + 1, :] * (-2.0 * time_step / 60.0), 0.0
        )
        high, low = split(wall)
        added = dot(high, row, TN) + dot(low, row, TN)
        at = slice(b * per, (b + 1) * per)
        next_out[0, at] = pressure_ref[at] + added.reshape(per, cells_y, length)


def exchange(value, devices, channels, chunk_rows, rows, capacity):
    if chunk_rows:
        shape = (devices, 1, channels * chunk_rows * LANES)
        got = lax.all_to_all(value.reshape(shape), AXES, split_axis=0, concat_axis=0, tiled=True)
        return got.reshape(channels * rows, LANES)
    value = value.reshape(channels, devices, capacity).transpose(1, 0, 2)
    got = lax.all_to_all(value, AXES, split_axis=0, concat_axis=0, tiled=True)
    return got.transpose(1, 0, 2).reshape(channels * rows, LANES)


def body(fluid_state, shell_disp, shell_vel, owners, node_local, rbf_weight, normals):
    span_count = lax.axis_size("span")
    chord_count = lax.axis_size("chord")
    devices = span_count * chord_count
    points, stencil = owners.shape
    capacity = max(2, (2 * points * stencil + devices - 1) // devices)
    rows = devices * capacity // LANES
    chunk_rows = capacity // LANES if capacity % LANES == 0 else 0
    blocks = points // LANES
    fields, cells_x, cells_y, length = fluid_state.shape
    _, nodes, width = shell_disp.shape
    sds = jax.ShapeDtypeStruct
    vmem = pl.BlockSpec(memory_space=pltpu.VMEM)
    hbm = pl.BlockSpec(memory_space=pl.ANY)

    near_out = pltpu.VMEM
    straight = 1
    span_shape = near_out((3 * fields + 1, cells_y, length), f32)
    chord_shape = near_out((2 * cells_x + 1, 8, length), f32)
    requests, dest, table, span_a, span_b, chord_a, chord_b = call(
        functools.partial(route_kernel, devices, capacity),
        [
            sds((rows, LANES), i32),
            near_out((stencil, points), i32),
            near_out(((6 - straight) * width, 2 * nodes), bf16),
            span_shape,
            span_shape,
            chord_shape,
            chord_shape,
        ],
        owners.T,
        node_local.T,
        shell_disp,
        shell_vel,
        fluid_state,
        flops=100_000_000,
        in_specs=[vmem, vmem, hbm, hbm, hbm],
        out_specs=[hbm] + [vmem] * 6,
        scratch_shapes=[
            pltpu.VMEM((rows, LANES), i32),
            pltpu.VMEM(shell_disp.shape, f32),
            pltpu.VMEM(shell_vel.shape, f32),
            pltpu.SemaphoreType.DMA((2 * fields + 7,)),
        ],
    )

    def swapped(one, two, axis, size):
        even = [pair for i in range(0, size - 1, 2) for pair in ((i, i + 1), (i + 1, i))]
        odd = [pair for i in range(1, size - 1, 2) for pair in ((i, i + 1), (i + 1, i))]
        first = lax.ppermute(one, axis, even)
        return first, lax.ppermute(two, axis, odd)

    got_xa, got_xb = swapped(span_a, span_b, "span", span_count)
    got_ya, got_yb = swapped(chord_a, chord_b, "chord", chord_count)

    asked = exchange(requests, devices, 1, chunk_rows, rows, capacity)

    slots = call(
        slots_kernel,
        near_out((3, rows, LANES), f32),
        dest,
        rbf_weight.T,
        held=(0,),
        flops=200_000_000,
    )
    flow_next, pressure, surface, shell_base = call(
        flow_kernel,
        [
            sds(fluid_state.shape, f32),
            near_out((cells_x, cells_y, length), f32),
            near_out((blocks, LANES), f32),
            near_out(shell_disp.shape, f32),
        ],
        shell_disp,
        shell_vel,
        fluid_state,
        got_xa,
        got_xb,
        got_ya,
        got_yb,
        flops=300_000_000,
        held=(0, 1, 3, 4, 5, 6),
        in_specs=[vmem, vmem, hbm, vmem, vmem, vmem, vmem],
        out_specs=[hbm, vmem, vmem, vmem],
        scratch_shapes=[
            pltpu.VMEM((fields, cells_x + 6, cells_y, length), f32),
            pltpu.VMEM((2, cells_x, cells_y, length), f32),
            pltpu.VMEM((2, cells_x, cells_y, length), f32),
            pltpu.VMEM((3, cells_x, cells_y, length), f32),
            pltpu.SemaphoreType.DMA((fields + 2,)),
        ],
    )

    picked = call(
        functools.partial(fetch_kernel, chunk_rows, 32),
        near_out((6 * rows, LANES), f32),
        asked,
        table,
        shell_disp,
        held=(0, 1, 2),
        flops=3_000_000_000,
    )
    replies = exchange(picked, devices, 6, chunk_rows, rows, capacity)

    wall_first = 2.0 * (-45.0 + 9.0 - 1.0) / 60.0
    group = 32
    wall, loads = call(
        functools.partial(meet_kernel, chunk_rows, group, -time_step * wall_first),
        [
            near_out((blocks, LANES), f32),
            sds((3 * rows, LANES), f32),
        ],
        replies,
        slots,
        surface,
        normals,
        held=(0, 1, 2, 3),
        flops=300_000_000,
        scratch_shapes=[pltpu.VMEM((rows // group, LANES, group * LANES), bf16)],
    )
    arrived = exchange(loads, devices, 3, chunk_rows, rows, capacity)

    block = pl.BlockSpec((1, cells_x, cells_y, length), lambda i: (0, 0, 0, 0))
    fluid_next, interface_motion = call(
        functools.partial(wall_kernel, chunk_rows, group),
        [sds(fluid_state.shape, f32), sds((6, points), f32)],
        replies,
        slots,
        wall,
        pressure,
        flow_next,
        flops=200_000_000,
        held=(0, 1, 2, 3),
        grid=(1,),
        in_specs=[vmem, vmem, vmem, vmem, hbm],
        out_specs=[block, vmem],
        input_output_aliases={4: 0},
    )

    disp_next, vel_next = call(
        functools.partial(force_kernel, chunk_rows, 64),
        [sds(shell_disp.shape, f32), sds(shell_vel.shape, f32)],
        arrived,
        asked,
        shell_base,
        shell_disp,
        held=(0, 1, 2, 3),
        flops=3_000_000_000,
        scratch_shapes=[pltpu.VMEM((3 * nodes, 2 * width), f32)],
    )
    return (fluid_next, interface_motion, disp_next, vel_next)


def solution(mesh):
    placed = (
        P(None, "span", "chord", None),
        P(None, "span", "chord"),
        P(None, "span", "chord"),
        P(AXES, None),
        P(AXES, None),
        P(AXES, None),
        P(None, AXES),
    )

    return jax.shard_map(
        body,
        mesh=mesh,
        in_specs=placed,
        out_specs=(
            P(None, "span", "chord", None),
            P(None, AXES),
            P(None, "span", "chord"),
            P(None, "span", "chord"),
        ),
        check_vma=False,
    )
```
